256 devices in a mesh: section: 8 (over y, x_lo), fork: 32 (over z, x_hi, core).
Axes of the slice: x: 4 (x_hi: 2, x_lo: 2; x = x_hi * 2 + x_lo), y: 4, z: 8, core: 2. Of those that a mesh axis runs over, the one named last changes fastest.
Arguments:
- arriving: bfloat16 [8, 32, 128, 4096], P('section', 'fork'), may hold values from -6 to 6
- saved_input: bfloat16 [8, 32, 128, 4096], P('section', 'fork'), may hold values from -6 to 6
- returning: bfloat16 [8, 32, 128, 4096], P('section', 'fork'), may hold values from -6 to 6
- prompt_cache: bfloat16 [8, 2, 2048, 512], P('section', None, 'fork'), may hold values from -20 to 20
- fresh_cache: bfloat16 [8, 32, 2, 128, 512], P('section', 'fork'), may hold values from -6 to 6
- back_cache: bfloat16 [8, 32, 2, 128, 512], P('section', 'fork'), may hold values from -6 to 6
- query_gain: float32 [8, 4096], P('section'), may hold values from 0.25 to 1.75
- block_tables: int32 [32, 64], P('fork'), may hold values from 0 to 127, as said below
- fresh_lengths: int32 [32], P('fork'), may hold values from 32 to 128
- back_lengths: int32 [32], P('fork'), may hold values from 32 to 128
Outputs:
- section_output: bfloat16 [8, 32, 128, 4096], P('section', 'fork')
- input_grad: bfloat16 [8, 32, 128, 4096], P('section', 'fork')
- prompt_grad: float32 [8, 2, 2048, 512], P('section', None, 'fork')
- completion_grad: float32 [8, 32, 2, 128, 512], P('section', 'fork')
- gain_grad: float32 [8, 4096], P('section')
The draws below stay inside these ranges and needn't reach their ends.
Inputs may be any that keep to these rules, and one draw needn't show every extreme that they name: `block_tables`: completions 0 to 15 read one prompt and the others a second one: each row lists that prompt's 64 pool blocks in order, the same row for all completions of a prompt; the two prompts' blocks are distinct and together fill the pool.
All inputs are finite; a program needn't handle non-finite values.
Results may differ from the reference program's by a relative error of at most 0.0023.
The reference program's roundings to bfloat16 on the way count: a program that leaves them out, or rounds other values in their place, can miss the bound.
Values may be sent and summed in bfloat16 or wider, within the bound.
No kernel may reach another device: no remote copies, remote signals or barrier semaphores. Data moves between devices by JAX's collectives and lax.ppermute only.
A program may use at most 128 MiB of HBM per device.

```python
import jax
import jax.numpy as jnp
from jax import lax

KV = 4
HD = 128
BLOCK = 16
COMP = 128
W = 4096
SECTIONS = 8
FORKS = 32
POOL = 128
NB = 64


def activation_draw(key, salt):
    shape = (SECTIONS, FORKS, COMP, W)
    base = jax.random.normal(jax.random.fold_in(key, salt), shape, jnp.float32)
    return jnp.clip(base, -6.0, 6.0)


def draw_arriving(key, part):
    return activation_draw(key, 101).astype(jnp.bfloat16)


def draw_saved_input(key, part):
    return activation_draw(key, 202).astype(jnp.bfloat16)


def draw_prompt_cache(key, part):
    shape = (SECTIONS, 2, POOL * BLOCK, KV * HD)
    base = jax.random.normal(jax.random.fold_in(key, 303), shape, jnp.float32)
    return jnp.clip(base, -6.0, 6.0).astype(jnp.bfloat16)


def draw_block_tables(key, part):
    shuffled = jax.random.permutation(jax.random.fold_in(key, 17), POOL)
    completion = jnp.arange(FORKS, dtype=jnp.int32)
    prompt_index = completion // (FORKS // 2)
    places = prompt_index[:, None] * NB + jnp.arange(NB, dtype=jnp.int32)[None, :]
    return shuffled[places].astype(jnp.int32)


def set_ends(entries, stream_key, low, top_value):
    longest = entries.shape.index(max(entries.shape))
    spots = []
    for shift in (0, 1):
        where = [jax.random.randint(jax.random.fold_in(stream_key, axis), (), 0, length) for axis, length in enumerate(entries.shape)]
        where[longest] = (where[longest] + shift) % entries.shape[longest]
        spots.append(tuple(where))
    return entries.at[spots[0]].set(low).at[spots[1]].set(top_value)


def steps_of(stream_key, dims, cuts, low, largest):
    def one(axis_at, parts):
        heights = jax.random.uniform(jax.random.fold_in(jax.random.fold_in(stream_key, 6), axis_at), (parts,), jnp.float32, low / len(cuts), largest / len(cuts))
        return jnp.repeat(jnp.exp(heights), dims[axis_at] // parts).reshape((-1,) + (1,) * (len(dims) - axis_at - 1))

    level = one(*cuts[0])
    for cut in cuts[1:]:
        level = level * one(*cut)
    return level


def bell_draw(own_key, extent, spread, reach, split=(), kind=jnp.bfloat16):
    entries = spread * jax.random.normal(own_key, extent, jnp.float32)
    if split:
        entries = entries * steps_of(own_key, extent, split, -0.22, 0.18)
    return jnp.clip(entries, -reach, reach).astype(kind)


def setup_inputs(seed: int = 0) -> dict:
    splits = jax.random.split(jax.random.key(seed), 11)
    return {
        "arriving": draw_arriving(jax.random.fold_in(splits[10], 71), 0),
        "saved_input": draw_saved_input(jax.random.fold_in(splits[10], 71), 0),
        "returning": bell_draw(splits[2], (SECTIONS, FORKS, COMP, W), 1.0, 6.0, ((0, 8), (1, 32))),
        "prompt_cache": draw_prompt_cache(jax.random.fold_in(splits[10], 71), 0),
        "fresh_cache": bell_draw(splits[4], (SECTIONS, FORKS, 2, COMP, KV * HD), 1.0, 6.0, ((0, 8), (1, 32))),
        "back_cache": bell_draw(splits[5], (SECTIONS, FORKS, 2, COMP, KV * HD), 1.0, 6.0, ((0, 8), (1, 32))),
        "query_gain": jnp.clip(1.0 + 0.15 * jax.random.normal(splits[6], (SECTIONS, W), jnp.float32), 0.25, 1.75),
        "block_tables": draw_block_tables(jax.random.fold_in(splits[10], 71), 0),
        "fresh_lengths": set_ends(jax.random.randint(splits[8], (FORKS,), COMP // 4, COMP + 1), jax.random.fold_in(splits[8], 1), COMP // 4, COMP).astype(jnp.int32),
        "back_lengths": set_ends(jax.random.randint(splits[9], (FORKS,), COMP // 4, COMP + 1), jax.random.fold_in(splits[9], 1), COMP // 4, COMP).astype(jnp.int32),
    }


epsilon = 1e-06
masked_score = -1e+30

def normed(x_rows, gain_row):
    floated = x_rows.astype(jnp.float32)
    inverse = lax.rsqrt(lax.optimization_barrier(jnp.mean(floated * floated, axis=-1, keepdims=True)) + epsilon)
    queries = lax.optimization_barrier((floated * inverse * gain_row).astype(jnp.bfloat16))
    return (queries, floated, inverse)

def visible_keys(row_count, prompt_count, length):
    places = jnp.arange(row_count, dtype=jnp.int32)
    recent = (places[None, :] <= places[:, None]) & (places[None, :] < length)
    return jnp.concatenate([jnp.ones((row_count, prompt_count), dtype=bool), recent], axis=1)

def by_group(array):
    return array.reshape(array.shape[0], KV, -1).transpose(1, 0, 2)

def softmax_rows(q_group, k_group, key_mask):
    row_count = q_group.shape[0]
    head_rows = q_group.reshape(row_count, -1, HD).astype(jnp.float32)
    scores = jnp.einsum('ihd,td->hit', head_rows, k_group.astype(jnp.float32)) * HD ** (-0.5)
    scores = jnp.where(key_mask[None], scores, masked_score)
    shifted = jnp.exp(scores - lax.optimization_barrier(jnp.max(scores, axis=-1, keepdims=True)))
    return (shifted / lax.optimization_barrier(jnp.sum(shifted, axis=-1, keepdims=True)), head_rows)

def forward_layer(x_rows, gain_row, prompt_keys, prompt_values, own_cache, length):
    queries, floated, inverse = normed(x_rows, gain_row)
    row_count = x_rows.shape[0]
    all_keys = jnp.concatenate([prompt_keys, own_cache[0]], axis=0)
    all_values = jnp.concatenate([prompt_values, own_cache[1]], axis=0)
    key_mask = visible_keys(row_count, prompt_keys.shape[0], length)

    def per_group(pieces):
        q_group, k_group, v_group = pieces
        chances, head_rows = softmax_rows(q_group, k_group, key_mask)
        rounded = lax.optimization_barrier(chances.astype(jnp.bfloat16)).astype(jnp.float32)
        return jnp.einsum('hit,td->ihd', rounded, v_group.astype(jnp.float32)).reshape(row_count, -1)
    results = lax.map(per_group, (by_group(queries), by_group(all_keys), by_group(all_values)))
    attended = results.transpose(1, 0, 2).reshape(row_count, -1)
    valid_rows = (jnp.arange(row_count, dtype=jnp.int32) < length).astype(jnp.float32)[:, None]
    return (floated + valid_rows * attended).astype(jnp.bfloat16)

def backward_layer(x_rows, gain_row, prompt_keys, prompt_values, own_cache, length, cotangent):
    queries, floated, inverse = normed(x_rows, gain_row)
    row_count = x_rows.shape[0]
    prompt_count = prompt_keys.shape[0]
    all_keys = jnp.concatenate([prompt_keys, own_cache[0]], axis=0)
    all_values = jnp.concatenate([prompt_values, own_cache[1]], axis=0)
    key_mask = visible_keys(row_count, prompt_count, length)
    valid_rows = (jnp.arange(row_count, dtype=jnp.int32) < length).astype(jnp.float32)[:, None]
    grad_float = cotangent.astype(jnp.float32)
    out_grad = lax.optimization_barrier((valid_rows * grad_float).astype(jnp.bfloat16))

    def per_group(pieces):
        q_group, k_group, v_group, d_group = pieces
        chances, head_rows = softmax_rows(q_group, k_group, key_mask)
        rounded = lax.optimization_barrier(chances.astype(jnp.bfloat16)).astype(jnp.float32)
        d_out = d_group.reshape(row_count, -1, HD).astype(jnp.float32)
        d_value = jnp.einsum('hit,ihd->td', rounded, d_out)
        d_weight = jnp.einsum('ihd,td->hit', d_out, v_group.astype(jnp.float32))
        row_delta = lax.optimization_barrier(jnp.sum(chances * d_weight, axis=-1, keepdims=True))
        d_score = (chances * (d_weight - row_delta) * HD ** (-0.5)).astype(jnp.bfloat16)
        d_score = lax.optimization_barrier(d_score).astype(jnp.float32)
        d_query = jnp.einsum('hit,td->ihd', d_score, k_group.astype(jnp.float32)).reshape(row_count, -1)
        d_key = jnp.einsum('hit,ihd->td', d_score, head_rows)
        return (d_query, d_key, d_value)
    d_query, d_key, d_value = lax.map(per_group, (by_group(queries), by_group(all_keys), by_group(all_values), by_group(out_grad)))
    d_query = d_query.transpose(1, 0, 2).reshape(row_count, -1)
    d_key = d_key.transpose(1, 0, 2).reshape(all_keys.shape[0], -1)
    d_value = d_value.transpose(1, 0, 2).reshape(all_keys.shape[0], -1)
    d_normed = d_query * gain_row
    d_input = inverse * d_normed - floated * inverse ** 3 * lax.optimization_barrier(jnp.mean(d_normed * floated, axis=-1, keepdims=True))
    gain_part = lax.optimization_barrier(jnp.sum(d_query * floated * inverse, axis=0))
    own_grad = jnp.stack([d_key[prompt_count:], d_value[prompt_count:]])
    shared_grad = jnp.stack([d_key[:prompt_count], d_value[:prompt_count]])
    return ((grad_float + d_input).astype(jnp.bfloat16), own_grad, shared_grad, gain_part)

def reference(arriving, saved_input, returning, prompt_cache, fresh_cache, back_cache, query_gain, block_tables, fresh_lengths, back_lengths):
    entering = jnp.roll(arriving, 1, axis=0)
    leaving = jnp.roll(returning, -1, axis=0)

    def section_step(unused, inputs):
        fresh_x, back_x, cotangents, block_pool, fresh_kv, back_kv, gain_row = inputs
        blocks = block_pool.reshape(2, -1, BLOCK, block_pool.shape[-1])

        def fork_step(running, member):
            pool_total, gain_total = running
            x_fresh, x_back, cot_rows, kv_fresh, kv_back, block_table, length_fresh, length_back = member
            picked = jnp.take(blocks, block_table, axis=1).reshape(2, -1, block_pool.shape[-1])
            out_fresh = forward_layer(x_fresh, gain_row, picked[0], picked[1], kv_fresh, length_fresh)
            out_back, own_grad, shared_grad, gain_part = backward_layer(x_back, gain_row, picked[0], picked[1], kv_back, length_back, cot_rows)
            pool_total = pool_total.at[:, block_table].add(shared_grad.reshape(2, block_table.shape[0], BLOCK, -1))
            return ((pool_total, gain_total + gain_part), (out_fresh, out_back, own_grad))
        start_state = (jnp.zeros(blocks.shape, jnp.float32), jnp.zeros(gain_row.shape, jnp.float32))
        (pool_total, gain_total), (out_fresh, out_back, own_grad) = lax.scan(fork_step, start_state, (fresh_x, back_x, cotangents, fresh_kv, back_kv, block_tables, fresh_lengths, back_lengths))
        return (unused, (out_fresh, out_back, pool_total.reshape(block_pool.shape), own_grad, gain_total))
    unused, results = lax.scan(section_step, jnp.zeros((), jnp.float32), (entering, saved_input, leaving, prompt_cache, fresh_cache, back_cache, query_gain))
    section_output, input_grad, prompt_grad, completion_grad, gain_grad = results
    return (section_output, input_grad, prompt_grad, completion_grad, gain_grad)
```

```python
import jax
import jax.numpy as jnp
from jax import lax
from jax.experimental import pallas as pl
from jax.experimental.pallas import tpu as pltpu
from jax.sharding import Mesh
from jax.sharding import PartitionSpec as P

KV = 4
HD = 128
BLOCK = 16
COMP = 128
NB = 64
GW = 1024
HEADS = 8
PROMPT = NB * BLOCK
SCALE = HD ** (-0.5)
FORK = ("fork_0", "fork_1", "fork_2")
QUAD = ("fork_1", "fork_2")
INTERPRET = False


epsilon = 1e-06
masked_score = -1e30
bf16 = jnp.bfloat16
f32 = jnp.float32

NT = (((1,), (1,)), ((), ()))

OWN_K, OWN_V, FRESH_K, FRESH_V, STATS = 1024, 1152, 1280, 1408, 1536
SAVED_W = 1664
ARRIVE_W = 1152


def nt_dot(a, b):
    return lax.dot_general(a, b, NT, preferred_element_type=f32)


def nn_dot(a, b):
    return jnp.dot(a, b, preferred_element_type=f32)


def stats_tile(x, lengths):
    floated = x.astype(f32)
    inverse = lax.rsqrt(jnp.mean(floated * floated, axis=-1, keepdims=True) + epsilon)
    high = inverse.astype(bf16).astype(f32)
    rest = inverse - high
    middle = rest.astype(bf16).astype(f32)
    low = rest - middle
    lane = lax.broadcasted_iota(jnp.int32, (x.shape[0], HD), 1)
    tile = jnp.where(lane == 0, high, jnp.where(lane == 1, middle, jnp.where(lane == 2, low, 0.0)))
    for place, length in enumerate(lengths):
        tile = jnp.where(lane == 3 + place, length.astype(f32), tile)
    return tile.astype(bf16)


def read_stats(tile):
    t = tile.astype(f32)
    inverse = t[:, 0:1] + t[:, 1:2] + t[:, 2:3]
    return inverse, t[:, 3:4]


def pack_saved_kernel(scalars, x_ref, back_ref, fresh_ref, *out_refs):
    k = scalars[NB]
    tile = stats_tile(x_ref[...], (scalars[NB + 1],))
    for r in range(KV):
        g = jnp.bitwise_xor(k, r)
        out_ref = out_refs[r]
        out_ref[:, 0:GW] = x_ref[:, pl.ds(pl.multiple_of(g * GW, GW), GW)]
        cols = pl.ds(pl.multiple_of(g * HD, HD), HD)
        out_ref[:, OWN_K : OWN_K + HD] = back_ref[0, :, cols]
        out_ref[:, OWN_V : OWN_V + HD] = back_ref[1, :, cols]
        out_ref[:, FRESH_K : FRESH_K + HD] = fresh_ref[0, :, cols]
        out_ref[:, FRESH_V : FRESH_V + HD] = fresh_ref[1, :, cols]
        out_ref[:, STATS : STATS + HD] = tile


def pack_returning_kernel(scalars, x_ref, *out_refs):
    k = scalars[NB]
    for r in range(KV):
        start = pl.multiple_of(jnp.bitwise_xor(k, r) * GW, GW)
        out_refs[r][...] = x_ref[:, pl.ds(start, GW)]


def pack_arriving_kernel(scalars, x_ref, *out_refs):
    k = scalars[NB]
    tile = stats_tile(x_ref[...], (scalars[NB + 2],))
    for r in range(KV):
        start = pl.multiple_of(jnp.bitwise_xor(k, r) * GW, GW)
        out_refs[r][:, 0:GW] = x_ref[:, pl.ds(start, GW)]
        out_refs[r][:, GW : GW + HD] = tile


def two_heads(rows, pair):
    a = 2 * pair * HD
    return jnp.concatenate([rows[:, a : a + HD], rows[:, a + HD : a + 2 * HD]], axis=0)


def own_mask(length):
    u = lax.broadcasted_iota(jnp.int32, (COMP, 2 * COMP), 0)
    i = lax.broadcasted_iota(jnp.int32, (COMP, 2 * COMP), 1) & (COMP - 1)
    return (u <= i) & (u.astype(f32) < length)


NCHUNK = (PROMPT + COMP) // HD


def softmax_columns(q2, keys_ref, s_ref, mask):
    top = None
    for c in range(NCHUNK):
        s = nt_dot(keys_ref[c * HD : (c + 1) * HD, :], q2) * SCALE
        if c == NCHUNK - 1:
            s = jnp.where(mask, s, masked_score)
        s_ref[c * HD : (c + 1) * HD, :] = s
        part = jnp.max(s, axis=0, keepdims=True)
        top = part if top is None else jnp.maximum(top, part)
    total = None
    for c in range(NCHUNK):
        p = jnp.exp(s_ref[c * HD : (c + 1) * HD, :] - top)
        s_ref[c * HD : (c + 1) * HD, :] = p
        part = jnp.sum(p, axis=0, keepdims=True)
        total = part if total is None else total + part
    return 1.0 / total


def put_by_step(j, out_refs, from_ref):
    for r in range(KV):

        @pl.when(j == r)
        def _(r=r):
            out_refs[r][...] = from_ref[...]


def backward_kernel(
    scalars, pool_ref, saved_ref, grad_ref, gain_ref,
    dq_ref, own_0, own_1, own_2, own_3, reduce_ref, k_out_ref, v_out_ref,
    keys_ref, keys_t_ref, values_ref, dk_ref, dv_ref, s_ref, w_ref, gain_acc, t_acc,
):
    j = pl.program_id(0)
    own_refs = (own_0, own_1, own_2, own_3)

    @pl.when(j == 0)
    def _():
        def pick(n, carry):
            b = scalars[n]
            member = b // 4
            at = pl.multiple_of((b % 4) * BLOCK, BLOCK)
            to = pl.multiple_of(n * BLOCK, BLOCK)
            keys_ref[pl.ds(to, BLOCK), :] = pool_ref[member, pl.ds(at, BLOCK), :]
            values_ref[pl.ds(to, BLOCK), :] = pool_ref[member, pl.ds(at + 64, BLOCK), :]
            return carry

        lax.fori_loop(0, NB, pick, 0)
        k_out_ref[...] = keys_ref[0:PROMPT, :]
        v_out_ref[...] = values_ref[0:PROMPT, :]
        for c in range(NCHUNK - 1):
            rows = slice(c * HD, (c + 1) * HD)
            keys_t_ref[:, rows] = keys_ref[rows, :].astype(f32).T.astype(bf16)
        dk_ref[0:PROMPT, :] = jnp.zeros((PROMPT, HD), f32)
        dv_ref[0:PROMPT, :] = jnp.zeros((PROMPT, HD), f32)
        gain_acc[...] = jnp.zeros(gain_acc.shape, f32)

    inverse, length = read_stats(saved_ref[0, :, STATS : STATS + HD])
    x = saved_ref[0, :, 0:GW].astype(f32)
    normal = x * inverse
    gain = gain_ref[...]
    q = (normal * gain).astype(bf16)
    row = lax.broadcasted_iota(jnp.int32, (COMP, 1), 0).astype(f32)
    valid = row < length
    d_out = jnp.where(valid, grad_ref[0].astype(f32), 0.0).astype(bf16)
    keys_ref[PROMPT:, :] = saved_ref[0, :, OWN_K : OWN_K + HD]
    values_ref[PROMPT:, :] = saved_ref[0, :, OWN_V : OWN_V + HD]
    keys_t_ref[:, PROMPT:] = saved_ref[0, :, OWN_K : OWN_K + HD].astype(f32).T.astype(bf16)
    dk_ref[PROMPT:, :] = jnp.zeros((COMP, HD), f32)
    dv_ref[PROMPT:, :] = jnp.zeros((COMP, HD), f32)
    mask = own_mask(length)

    t = jnp.zeros((COMP, 1), f32)
    for pair in range(HEADS // 2):
        q2 = two_heads(q, pair)
        d2 = two_heads(d_out, pair)
        ratio = softmax_columns(q2, keys_ref, s_ref, mask)
        delta = None
        for c in range(NCHUNK):
            rows = slice(c * HD, (c + 1) * HD)
            a = s_ref[rows, :] * ratio
            s_ref[rows, :] = a
            dv_ref[rows, :] += nn_dot(a.astype(bf16), d2)
            dw = nt_dot(values_ref[rows, :], d2)
            w_ref[rows, :] = dw
            part = jnp.sum(a * dw, axis=0, keepdims=True)
            delta = part if delta is None else delta + part
        dq_t = None
        for c in range(NCHUNK):
            rows = slice(c * HD, (c + 1) * HD)
            ds = (s_ref[rows, :] * (w_ref[rows, :] - delta) * SCALE).astype(bf16)
            dk_ref[rows, :] += nn_dot(ds, q2)
            part = nn_dot(keys_t_ref[:, rows], ds)
            dq_t = part if dq_t is None else dq_t + part
        for e in range(2):
            h = 2 * pair + e
            cols = slice(h * HD, (h + 1) * HD)
            dq = dq_t[:, e * HD : (e + 1) * HD].T
            dq_ref[0, :, cols] = dq
            t = t + jnp.sum(dq * gain[:, cols] * x[:, cols], axis=1, keepdims=True)
            gain_acc[h : h + 1, :] += jnp.sum(dq * normal[:, cols], axis=0, keepdims=True)

    for r in range(KV):

        @pl.when(j == r)
        def _(r=r):
            own_refs[r][0:COMP, :] = dk_ref[PROMPT:, :]
            own_refs[r][COMP : 2 * COMP, :] = dv_ref[PROMPT:, :]

    place = pl.multiple_of(jnp.bitwise_xor(j, scalars[NB]) * 8, 8)
    t_acc[pl.ds(place, 8), :] = jnp.broadcast_to(t, (COMP, HD)).T[0:8, :]

    @pl.when(j == KV - 1)
    def _():
        for place in range(KV):
            for m in range(KV):
                own_refs[m][2 * COMP + place : 2 * COMP + place + 1, :] = t_acc[place * 8 : place * 8 + 1, :]
            own_refs[place][2 * COMP + 4 : 2 * COMP + 8, :] = jnp.zeros((4, HD), f32)
        high = gain_acc[...].astype(bf16)
        low = (gain_acc[...] - high.astype(f32)).astype(bf16)
        both = jnp.concatenate([high, low], axis=0)

        def clear(n, carry):
            reduce_ref[n, 0:HD, :] = jnp.zeros((HD, HD), bf16)
            reduce_ref[n, HD : HD + 16, :] = both
            return carry

        lax.fori_loop(0, 32, clear, 0)

        def spread(n, carry):
            b = scalars[n]
            member = b // 4
            at = pl.multiple_of((b % 4) * BLOCK, BLOCK)
            start = pl.multiple_of(n * BLOCK, BLOCK)
            reduce_ref[member, pl.ds(at, BLOCK), :] = dk_ref[pl.ds(start, BLOCK), :].astype(bf16)
            reduce_ref[member, pl.ds(at + 64, BLOCK), :] = dv_ref[pl.ds(start, BLOCK), :].astype(bf16)
            return carry

        lax.fori_loop(0, NB, spread, 0)


def forward_kernel(
    scalars, arrive_ref, saved_ref, prompt_k_ref, prompt_v_ref, gain_ref,
    out_0, out_1, out_2, out_3, keys_ref, values_t_ref, s_ref, y_ref,
):
    j = pl.program_id(0)

    @pl.when(j == 0)
    def _():
        keys_ref[0:PROMPT, :] = prompt_k_ref[...]
        for c in range(NCHUNK - 1):
            rows = slice(c * HD, (c + 1) * HD)
            values_t_ref[:, rows] = prompt_v_ref[rows, :].astype(f32).T.astype(bf16)

    inverse, length = read_stats(arrive_ref[0, :, GW : GW + HD])
    x = arrive_ref[0, :, 0:GW].astype(f32)
    q = (x * inverse * gain_ref[...]).astype(bf16)
    row = lax.broadcasted_iota(jnp.int32, (COMP, 1), 0).astype(f32)
    valid = row < length
    keys_ref[PROMPT:, :] = saved_ref[0, :, FRESH_K : FRESH_K + HD]
    values_t_ref[:, PROMPT:] = saved_ref[0, :, FRESH_V : FRESH_V + HD].astype(f32).T.astype(bf16)
    mask = own_mask(length)
    for pair in range(HEADS // 2):
        q2 = two_heads(q, pair)
        ratio = softmax_columns(q2, keys_ref, s_ref, mask)
        o_t = None
        for c in range(NCHUNK):
            rows = slice(c * HD, (c + 1) * HD)
            w = (s_ref[rows, :] * ratio).astype(bf16)
            part = nn_dot(values_t_ref[:, rows], w)
            o_t = part if o_t is None else o_t + part
        for e in range(2):
            h = 2 * pair + e
            cols = slice(h * HD, (h + 1) * HD)
            o = jnp.where(valid, o_t[:, e * HD : (e + 1) * HD].T, 0.0)
            y_ref[:, cols] = (x[:, cols] + o).astype(bf16)
    put_by_step(j, (out_0, out_1, out_2, out_3), y_ref)


def input_grad_kernel(
    scalars, dq_ref, saved_ref, grad_ref, gain_ref, t_ref, out_0, out_1, out_2, out_3, y_ref
):
    j = pl.program_id(0)
    inverse, _ = read_stats(saved_ref[0, :, STATS : STATS + HD])
    total = t_ref[0] + t_ref[1] + t_ref[2] + t_ref[3]
    place = lax.broadcasted_iota(jnp.int32, (8, HD), 0)
    t_row = jnp.sum(jnp.where(place == jnp.bitwise_xor(j, scalars[NB]), total, 0.0), axis=0, keepdims=True)
    t = jnp.broadcast_to(t_row, (HD, HD)).T[:, 0:1] * (1.0 / (KV * GW))
    x = saved_ref[0, :, 0:GW].astype(f32)
    dx = inverse * (dq_ref[0] * gain_ref[...]) - x * (inverse * inverse * inverse * t)
    y_ref[...] = (grad_ref[0].astype(f32) + dx).astype(bf16)
    put_by_step(j, (out_0, out_1, out_2, out_3), y_ref)


def pool_sum_kernel(got_ref, out_ref, gain_ref):
    for g in range(KV):
        total = got_ref[g].astype(f32)
        for z in range(1, 8):
            total = total + got_ref[z * KV + g].astype(f32)
        cols = slice(g * HD, (g + 1) * HD)
        out_ref[0, :, cols] = total[0:64, :]
        out_ref[1, :, cols] = total[64:128, :]
        gain_ref[g] = total[128:136, :] + total[136:144, :]


def join_rows_kernel(scalars, *refs):
    out_ref = refs[KV]
    for r in range(KV):
        start = pl.multiple_of(jnp.bitwise_xor(scalars[NB], r) * GW, GW)
        out_ref[:, pl.ds(start, GW)] = refs[r][...]


def join_own_kernel(scalars, *refs):
    out_ref = refs[KV]
    for r in range(KV):
        cols = pl.ds(pl.multiple_of(jnp.bitwise_xor(scalars[NB], r) * HD, HD), HD)
        out_ref[0, :, cols] = refs[r][0:COMP, :]
        out_ref[1, :, cols] = refs[r][COMP : 2 * COMP, :]


smem = pl.BlockSpec(memory_space=pltpu.SMEM)
vmem = pl.BlockSpec(memory_space=pltpu.VMEM)


def whole(kernel, out_shape, in_specs):
    count = len(out_shape) if isinstance(out_shape, (list, tuple)) else None
    return pl.pallas_call(
        kernel,
        out_shape=out_shape,
        in_specs=in_specs,
        out_specs=[vmem] * count if count else vmem,
        interpret=INTERPRET,
    )


def shifted_to_group(values, steps):
    sections = lax.axis_size("section")
    got = []
    for r, value in enumerate(values):
        pairs = [
            (s * KV + k, ((s + steps) % sections) * KV + (k ^ r))
            for s in range(sections)
            for k in range(KV)
        ]
        got.append(lax.ppermute(value, ("section",) + QUAD, pairs))
    return jnp.stack(got)


def exchanged(values):
    pairs = lambda r: [(k, k ^ r) for k in range(KV)]
    return [values[0]] + [lax.ppermute(values[r], QUAD, pairs(r)) for r in range(1, KV)]


def to_all(tiles):
    return lax.all_to_all(tiles, FORK, 0, 0, tiled=True)


def by_member(shape):
    return pl.BlockSpec((1,) + shape, lambda j, scalars: (j,) + (0,) * len(shape))


def fixed(shape):
    return pl.BlockSpec(shape, lambda j, scalars: (0,) * len(shape))


gain_spec = pl.BlockSpec((1, GW), lambda j, scalars: (0, scalars[NB]))


def over_members(kernel, in_specs, out_specs, out_shape, scratch, flops):
    return pl.pallas_call(
        kernel,
        out_shape=out_shape,
        grid_spec=pltpu.PrefetchScalarGridSpec(
            num_scalar_prefetch=1,
            grid=(KV,),
            in_specs=in_specs,
            out_specs=out_specs,
            scratch_shapes=scratch,
        ),
        compiler_params=pltpu.CompilerParams(dimension_semantics=("arbitrary",)),
        cost_estimate=pl.CostEstimate(flops=flops, transcendentals=0, bytes_accessed=4 << 20),
        interpret=INTERPRET,
    )


def shaped(shape, dtype):
    return jax.ShapeDtypeStruct(shape, dtype)


def section_tick(
    arriving,
    saved_input,
    returning,
    prompt_cache,
    fresh_cache,
    back_cache,
    query_gain,
    block_tables,
    fresh_lengths,
    back_lengths,
):
    member = 2 * lax.axis_index("fork_1") + lax.axis_index("fork_2")
    scalars = jnp.concatenate(
        [
            block_tables[0],
            member.astype(jnp.int32)[None],
            back_lengths,
            fresh_lengths,
            jnp.zeros((5,), jnp.int32),
        ]
    )
    keys = PROMPT + COMP
    four = range(KV)

    pool = prompt_cache[0].reshape(2, 64, KV, HD).transpose(2, 0, 1, 3).reshape(1, KV, HD, HD)
    pool = jnp.broadcast_to(pool, (8, KV, HD, HD)).reshape(32, HD, HD)
    pool = to_all(pool)

    saved = whole(
        pack_saved_kernel, [shaped((COMP, SAVED_W), bf16)] * KV, [smem, vmem, vmem, vmem]
    )(scalars, saved_input[0, 0], back_cache[0, 0], fresh_cache[0, 0])
    saved = jnp.stack(exchanged(saved))

    cotangent = whole(
        pack_returning_kernel, [shaped((COMP, GW), bf16)] * KV, [smem, vmem]
    )(scalars, returning[0, 0])
    cotangent = shifted_to_group(cotangent, -1)
    incoming = whole(
        pack_arriving_kernel, [shaped((COMP, ARRIVE_W), bf16)] * KV, [smem, vmem]
    )(scalars, arriving[0, 0])
    incoming = shifted_to_group(incoming, 1)

    d_query, *own, reduced, prompt_k, prompt_v = over_members(
        backward_kernel,
        [fixed((32, HD, HD)), by_member((COMP, SAVED_W)), by_member((COMP, GW)), gain_spec],
        [by_member((COMP, GW))]
        + [fixed((2 * COMP + 8, HD)) for _ in four]
        + [fixed((32, 144, HD)), fixed((PROMPT, HD)), fixed((PROMPT, HD))],
        [shaped((KV, COMP, GW), f32)]
        + [shaped((2 * COMP + 8, HD), f32) for _ in four]
        + [shaped((32, 144, HD), bf16), shaped((PROMPT, HD), bf16), shaped((PROMPT, HD), bf16)],
        [
            pltpu.VMEM((keys, HD), bf16),
            pltpu.VMEM((HD, keys), bf16),
            pltpu.VMEM((keys, HD), bf16),
            pltpu.VMEM((keys, HD), f32),
            pltpu.VMEM((keys, HD), f32),
            pltpu.VMEM((keys, 2 * COMP), f32),
            pltpu.VMEM((keys, 2 * COMP), f32),
            pltpu.VMEM((HEADS, HD), f32),
            pltpu.VMEM((32, HD), f32),
        ],
        10 * 4096 * keys * HD,
    )(scalars, pool, saved, cotangent, query_gain)

    reduced = to_all(reduced)
    own = exchanged(own)

    output = over_members(
        forward_kernel,
        [
            by_member((COMP, ARRIVE_W)),
            by_member((COMP, SAVED_W)),
            fixed((PROMPT, HD)),
            fixed((PROMPT, HD)),
            gain_spec,
        ],
        [fixed((COMP, GW)) for _ in four],
        [shaped((COMP, GW), bf16) for _ in four],
        [
            pltpu.VMEM((keys, HD), bf16),
            pltpu.VMEM((HD, keys), bf16),
            pltpu.VMEM((keys, 2 * COMP), f32),
            pltpu.VMEM((COMP, GW), bf16),
        ],
        4 * 4096 * keys * HD,
    )(scalars, incoming, saved, prompt_k, prompt_v, query_gain)
    output = exchanged(output)

    input_grad = over_members(
        input_grad_kernel,
        [
            by_member((COMP, GW)),
            by_member((COMP, SAVED_W)),
            by_member((COMP, GW)),
            gain_spec,
            fixed((KV, 8, HD)),
        ],
        [fixed((COMP, GW)) for _ in four],
        [shaped((COMP, GW), bf16) for _ in four],
        [pltpu.VMEM((COMP, GW), bf16)],
        1 << 20,
    )(scalars, d_query, saved, cotangent, query_gain, jnp.stack([tile[2 * COMP :] for tile in own]))
    input_grad = exchanged(input_grad)

    prompt_grad, gain_grad = whole(
        pool_sum_kernel, [shaped((2, 64, KV * HD), f32), shaped((KV, HEADS, HD), f32)], [vmem]
    )(reduced)

    joined = [smem] + [vmem] * KV
    rows = shaped((COMP, KV * GW), bf16)
    own_grad = whole(join_own_kernel, shaped((2, COMP, KV * HD), f32), joined)(scalars, *own)
    output = whole(join_rows_kernel, rows, joined)(scalars, *output)
    input_grad = whole(join_rows_kernel, rows, joined)(scalars, *input_grad)
    return (
        output[None, None],
        input_grad[None, None],
        prompt_grad[None],
        own_grad[None, None],
        gain_grad.reshape(1, KV * GW),
    )


def solution(mesh):
    finer = Mesh(
        mesh.devices.reshape(mesh.shape["section"], 8, 2, 2),
        ("section", "fork_0", "fork_1", "fork_2"),
    )
    placed = (
        P("section", FORK, None, None),
        P("section", FORK, None, None),
        P("section", FORK, None, None),
        P("section", None, FORK, None),
        P("section", FORK, None, None, None),
        P("section", FORK, None, None, None),
        P("section", None),
        P(FORK, None),
        P(FORK),
        P(FORK),
    )
    return jax.shard_map(
        section_tick,
        mesh=finer,
        in_specs=placed,
        out_specs=(
            P("section", FORK, None, None),
            P("section", FORK, None, None),
            P("section", None, FORK, None),
            P("section", FORK, None, None, None),
            P("section", None),
        ),
        check_vma=False,
    )
```

```python
import jax
import jax.numpy as jnp
from jax import lax
from jax.experimental import pallas as pl
from jax.experimental.pallas import tpu as pltpu
from jax.sharding import Mesh
from jax.sharding import PartitionSpec as P

KV = 4
HD = 128
BLOCK = 16
COMP = 128
NB = 64
GW = 1024
HEADS = 8
PROMPT = NB * BLOCK
SCALE = HD ** (-0.5)
FORK = ("fork_0", "fork_1", "fork_2")
QUAD = ("fork_1", "fork_2")
INTERPRET = False


epsilon = 1e-06
masked_score = -1e30
bf16 = jnp.bfloat16
f32 = jnp.float32

NT = (((1,), (1,)), ((), ()))

OWN_K, OWN_V, STATS = 1024, 1152, 1280
SAVED_W = 1408
ARRIVE_W = 1152
FIRST_ROWS = 384


def nt_dot(a, b):
    return lax.dot_general(a, b, NT, preferred_element_type=f32)


def nn_dot(a, b):
    return jnp.dot(a, b, preferred_element_type=f32)


def stats_tile(x, length):
    floated = x.astype(f32)
    inverse = lax.rsqrt(jnp.mean(floated * floated, axis=-1, keepdims=True) + epsilon)
    high = inverse.astype(bf16).astype(f32)
    rest = inverse - high
    middle = rest.astype(bf16).astype(f32)
    low = rest - middle
    lane = lax.broadcasted_iota(jnp.int32, (x.shape[0], HD), 1)
    tile = jnp.where(lane == 0, high, jnp.where(lane == 1, middle, jnp.where(lane == 2, low, 0.0)))
    tile = jnp.where(lane == 3, length.astype(f32), tile)
    return tile.astype(bf16)


def read_stats(tile):
    t = tile.astype(f32)
    inverse = t[:, 0:1] + t[:, 1:2] + t[:, 2:3]
    return inverse, t[:, 3:4]


def group_at(member, r, width):
    return pl.ds(pl.multiple_of(jnp.bitwise_xor(member[0], r) * width, width), width)


def pack_first_kernel(member, pool_ref, fresh_ref, *out_refs):
    for r in range(KV):
        cols = group_at(member, r, HD)
        out_refs[r][0:64, :] = pool_ref[0, :, cols]
        out_refs[r][64:128, :] = pool_ref[1, :, cols]
        out_refs[r][128:256, :] = fresh_ref[0, :, cols]
        out_refs[r][256:384, :] = fresh_ref[1, :, cols]


def pack_saved_kernel(member, length, x_ref, back_ref, *out_refs):
    tile = stats_tile(x_ref[...], length[0])
    for r in range(KV):
        out_ref = out_refs[r]
        out_ref[:, 0:GW] = x_ref[:, group_at(member, r, GW)]
        cols = group_at(member, r, HD)
        out_ref[:, OWN_K : OWN_K + HD] = back_ref[0, :, cols]
        out_ref[:, OWN_V : OWN_V + HD] = back_ref[1, :, cols]
        out_ref[:, STATS : STATS + HD] = tile


def pack_returning_kernel(member, x_ref, *out_refs):
    for r in range(KV):
        out_refs[r][...] = x_ref[:, group_at(member, r, GW)]


def pack_arriving_kernel(member, length, x_ref, *out_refs):
    tile = stats_tile(x_ref[...], length[0])
    for r in range(KV):
        out_refs[r][:, 0:GW] = x_ref[:, group_at(member, r, GW)]
        out_refs[r][:, GW : GW + HD] = tile


def two_heads(rows, pair):
    a = 2 * pair * HD
    return jnp.concatenate([rows[:, a : a + HD], rows[:, a + HD : a + 2 * HD]], axis=0)


def own_mask(length):
    u = lax.broadcasted_iota(jnp.int32, (COMP, 2 * COMP), 0)
    i = lax.broadcasted_iota(jnp.int32, (COMP, 2 * COMP), 1) & (COMP - 1)
    return (u <= i) & (u.astype(f32) < length)


NCHUNK = (PROMPT + COMP) // HD


def softmax_columns(q2, keys_ref, s_ref, mask):
    top = None
    for c in range(NCHUNK):
        s = nt_dot(keys_ref[c * HD : (c + 1) * HD, :], q2) * SCALE
        if c == NCHUNK - 1:
            s = jnp.where(mask, s, masked_score)
        s_ref[c * HD : (c + 1) * HD, :] = s
        part = jnp.max(s, axis=0, keepdims=True)
        top = part if top is None else jnp.maximum(top, part)
    total = None
    for c in range(NCHUNK):
        p = jnp.exp(s_ref[c * HD : (c + 1) * HD, :] - top)
        s_ref[c * HD : (c + 1) * HD, :] = p
        part = jnp.sum(p, axis=0, keepdims=True)
        total = part if total is None else total + part
    return 1.0 / total


def put_by_step(j, out_refs, from_ref):
    for r in range(KV):

        @pl.when(j == r)
        def _(r=r):
            out_refs[r][...] = from_ref[...]


def take_by_step(j, from_refs, to_ref):
    for r in range(KV):

        @pl.when(j == r)
        def _(r=r):
            to_ref[...] = from_refs[r][...]


def backward_kernel(
    member, table, saved_0, saved_1, saved_2, saved_3, grad_0, grad_1, grad_2, grad_3,
    prompt_k_ref, prompt_v_ref, gain_ref,
    dq_ref, own_0, own_1, own_2, own_3, reduce_ref,
    saved_ref, grad_ref,
    keys_ref, keys_t_ref, values_ref, dk_ref, dv_ref, s_ref, w_ref, gain_acc, t_acc,
):
    j = pl.program_id(0)
    own_refs = (own_0, own_1, own_2, own_3)
    take_by_step(j, (saved_0, saved_1, saved_2, saved_3), saved_ref)
    take_by_step(j, (grad_0, grad_1, grad_2, grad_3), grad_ref)

    @pl.when(j == 0)
    def _():
        keys_ref[0:PROMPT, :] = prompt_k_ref[...]
        values_ref[0:PROMPT, :] = prompt_v_ref[...]
        for c in range(NCHUNK - 1):
            rows = slice(c * HD, (c + 1) * HD)
            keys_t_ref[:, rows] = keys_ref[rows, :].astype(f32).T.astype(bf16)
        dk_ref[0:PROMPT, :] = jnp.zeros((PROMPT, HD), f32)
        dv_ref[0:PROMPT, :] = jnp.zeros((PROMPT, HD), f32)
        gain_acc[...] = jnp.zeros(gain_acc.shape, f32)

    inverse, length = read_stats(saved_ref[:, STATS : STATS + HD])
    x = saved_ref[:, 0:GW].astype(f32)
    normal = x * inverse
    gain = gain_ref[...]
    q = (normal * gain).astype(bf16)
    row = lax.broadcasted_iota(jnp.int32, (COMP, 1), 0).astype(f32)
    valid = row < length
    d_out = jnp.where(valid, grad_ref[...].astype(f32), 0.0).astype(bf16)
    keys_ref[PROMPT:, :] = saved_ref[:, OWN_K : OWN_K + HD]
    values_ref[PROMPT:, :] = saved_ref[:, OWN_V : OWN_V + HD]
    keys_t_ref[:, PROMPT:] = saved_ref[:, OWN_K : OWN_K + HD].astype(f32).T.astype(bf16)
    dk_ref[PROMPT:, :] = jnp.zeros((COMP, HD), f32)
    dv_ref[PROMPT:, :] = jnp.zeros((COMP, HD), f32)
    mask = own_mask(length)

    t = jnp.zeros((COMP, 1), f32)
    for pair in range(HEADS // 2):
        q2 = two_heads(q, pair)
        d2 = two_heads(d_out, pair)
        ratio = softmax_columns(q2, keys_ref, s_ref, mask)
        delta = None
        for c in range(NCHUNK):
            rows = slice(c * HD, (c + 1) * HD)
            a = s_ref[rows, :] * ratio
            s_ref[rows, :] = a
            dv_ref[rows, :] += nn_dot(a.astype(bf16), d2)
            dw = nt_dot(values_ref[rows, :], d2)
            w_ref[rows, :] = dw
            part = jnp.sum(a * dw, axis=0, keepdims=True)
            delta = part if delta is None else delta + part
        dq_t = None
        for c in range(NCHUNK):
            rows = slice(c * HD, (c + 1) * HD)
            ds = (s_ref[rows, :] * (w_ref[rows, :] - delta) * SCALE).astype(bf16)
            dk_ref[rows, :] += nn_dot(ds, q2)
            part = nn_dot(keys_t_ref[:, rows], ds)
            dq_t = part if dq_t is None else dq_t + part
        for e in range(2):
            h = 2 * pair + e
            cols = slice(h * HD, (h + 1) * HD)
            dq = dq_t[:, e * HD : (e + 1) * HD].T
            dq_ref[0, :, cols] = dq
            t = t + jnp.sum(dq * gain[:, cols] * x[:, cols], axis=1, keepdims=True)
            gain_acc[h : h + 1, :] += jnp.sum(dq * normal[:, cols], axis=0, keepdims=True)

    for r in range(KV):

        @pl.when(j == r)
        def _(r=r):
            own_refs[r][0:COMP, :] = dk_ref[PROMPT:, :]
            own_refs[r][COMP : 2 * COMP, :] = dv_ref[PROMPT:, :]

    place = pl.multiple_of(jnp.bitwise_xor(j, member[0]) * 8, 8)
    t_acc[pl.ds(place, 8), :] = jnp.broadcast_to(t, (COMP, HD)).T[0:8, :]

    @pl.when(j == KV - 1)
    def _():
        for place in range(KV):
            for m in range(KV):
                own_refs[m][2 * COMP + place : 2 * COMP + place + 1, :] = t_acc[place * 8 : place * 8 + 1, :]
            own_refs[place][2 * COMP + 4 : 2 * COMP + 8, :] = jnp.zeros((4, HD), f32)
        high = gain_acc[...].astype(bf16)
        low = (gain_acc[...] - high.astype(f32)).astype(bf16)
        both = jnp.concatenate([high, low], axis=0)

        def clear(n, carry):
            reduce_ref[n, 0:HD, :] = jnp.zeros((HD, HD), bf16)
            reduce_ref[n, HD : HD + 16, :] = both
            return carry

        lax.fori_loop(0, 32, clear, 0)

        def spread(n, carry):
            b = table[n]
            holder = b // 4
            at = pl.multiple_of((b % 4) * BLOCK, BLOCK)
            start = pl.multiple_of(n * BLOCK, BLOCK)
            reduce_ref[holder, pl.ds(at, BLOCK), :] = dk_ref[pl.ds(start, BLOCK), :].astype(bf16)
            reduce_ref[holder, pl.ds(at + 64, BLOCK), :] = dv_ref[pl.ds(start, BLOCK), :].astype(bf16)
            return carry

        lax.fori_loop(0, NB, spread, 0)


def forward_kernel(
    member, table, pool_ref, arrive_0, arrive_1, arrive_2, arrive_3,
    first_0, first_1, first_2, first_3, gain_ref,
    out_0, out_1, out_2, out_3, prompt_k_ref, prompt_v_ref,
    arrive_ref, first_ref, keys_ref, values_t_ref, s_ref, y_ref,
):
    j = pl.program_id(0)
    take_by_step(j, (arrive_0, arrive_1, arrive_2, arrive_3), arrive_ref)
    take_by_step(j, (first_0, first_1, first_2, first_3), first_ref)

    @pl.when(j == 0)
    def _():
        def pick(n, carry):
            b = table[n]
            place = (b // 16) * KV + jnp.bitwise_xor((b // 4) % 4, member[0])
            at = pl.multiple_of((b % 4) * BLOCK, BLOCK)
            to = pl.multiple_of(n * BLOCK, BLOCK)
            prompt_k_ref[pl.ds(to, BLOCK), :] = pool_ref[place, pl.ds(at, BLOCK), :]
            prompt_v_ref[pl.ds(to, BLOCK), :] = pool_ref[place, pl.ds(at + 64, BLOCK), :]
            return carry

        lax.fori_loop(0, NB, pick, 0)
        keys_ref[0:PROMPT, :] = prompt_k_ref[...]
        for c in range(NCHUNK - 1):
            rows = slice(c * HD, (c + 1) * HD)
            values_t_ref[:, rows] = prompt_v_ref[rows, :].astype(f32).T.astype(bf16)

    inverse, length = read_stats(arrive_ref[:, GW : GW + HD])
    x = arrive_ref[:, 0:GW].astype(f32)
    q = (x * inverse * gain_ref[...]).astype(bf16)
    row = lax.broadcasted_iota(jnp.int32, (COMP, 1), 0).astype(f32)
    valid = row < length
    keys_ref[PROMPT:, :] = first_ref[128:256, :]
    values_t_ref[:, PROMPT:] = first_ref[256:384, :].astype(f32).T.astype(bf16)
    mask = own_mask(length)
    for pair in range(HEADS // 2):
        q2 = two_heads(q, pair)
        ratio = softmax_columns(q2, keys_ref, s_ref, mask)
        o_t = None
        for c in range(NCHUNK):
            rows = slice(c * HD, (c + 1) * HD)
            w = (s_ref[rows, :] * ratio).astype(bf16)
            part = nn_dot(values_t_ref[:, rows], w)
            o_t = part if o_t is None else o_t + part
        for e in range(2):
            h = 2 * pair + e
            cols = slice(h * HD, (h + 1) * HD)
            o = jnp.where(valid, o_t[:, e * HD : (e + 1) * HD].T, 0.0)
            y_ref[:, cols] = (x[:, cols] + o).astype(bf16)
    put_by_step(j, (out_0, out_1, out_2, out_3), y_ref)


def input_grad_kernel(
    member, dq_ref, saved_0, saved_1, saved_2, saved_3, grad_0, grad_1, grad_2, grad_3,
    gain_ref, t_0, t_1, t_2, t_3, out_0, out_1, out_2, out_3, y_ref, saved_ref, grad_ref
):
    j = pl.program_id(0)
    take_by_step(j, (saved_0, saved_1, saved_2, saved_3), saved_ref)
    take_by_step(j, (grad_0, grad_1, grad_2, grad_3), grad_ref)
    inverse, _ = read_stats(saved_ref[:, STATS : STATS + HD])
    total = t_0[...] + t_1[...] + t_2[...] + t_3[...]
    place = lax.broadcasted_iota(jnp.int32, (8, HD), 0)
    t_row = jnp.sum(jnp.where(place == jnp.bitwise_xor(j, member[0]), total, 0.0), axis=0, keepdims=True)
    t = jnp.broadcast_to(t_row, (HD, HD)).T[:, 0:1] * (1.0 / (KV * GW))
    x = saved_ref[:, 0:GW].astype(f32)
    dx = inverse * (dq_ref[0] * gain_ref[...]) - x * (inverse * inverse * inverse * t)
    y_ref[...] = (grad_ref[...].astype(f32) + dx).astype(bf16)
    put_by_step(j, (out_0, out_1, out_2, out_3), y_ref)


def pool_sum_kernel(got_ref, out_ref, gain_ref):
    for g in range(KV):
        total = got_ref[g].astype(f32)
        for z in range(1, 8):
            total = total + got_ref[z * KV + g].astype(f32)
        cols = slice(g * HD, (g + 1) * HD)
        out_ref[0, :, cols] = total[0:64, :]
        out_ref[1, :, cols] = total[64:128, :]
        gain_ref[g] = total[128:136, :] + total[136:144, :]


def join_rows_kernel(member, *refs):
    out_ref = refs[KV]
    for r in range(KV):
        out_ref[:, group_at(member, r, GW)] = refs[r][...]


def join_own_kernel(member, *refs):
    out_ref = refs[KV]
    for r in range(KV):
        cols = group_at(member, r, HD)
        out_ref[0, :, cols] = refs[r][0:COMP, :]
        out_ref[1, :, cols] = refs[r][COMP : 2 * COMP, :]


smem = pl.BlockSpec(memory_space=pltpu.SMEM)
vmem = pl.BlockSpec(memory_space=pltpu.VMEM)


def whole(kernel, out_shape, in_specs):
    count = len(out_shape) if isinstance(out_shape, (list, tuple)) else None
    return pl.pallas_call(
        kernel,
        out_shape=out_shape,
        in_specs=in_specs,
        out_specs=[vmem] * count if count else vmem,
        interpret=INTERPRET,
    )


def shifted_to_group(values, steps):
    sections = lax.axis_size("section")
    got = []
    for r, value in enumerate(values):
        pairs = [
            (s * KV + k, ((s + steps) % sections) * KV + (k ^ r))
            for s in range(sections)
            for k in range(KV)
        ]
        got.append(lax.ppermute(value, ("section",) + QUAD, pairs))
    return got


def exchanged(values):
    pairs = lambda r: [(k, k ^ r) for k in range(KV)]
    return [values[0]] + [lax.ppermute(values[r], QUAD, pairs(r)) for r in range(1, KV)]


def to_all(tiles, axes):
    return lax.all_to_all(tiles, axes, 0, 0, tiled=True)


def by_member(shape):
    return pl.BlockSpec((1,) + shape, lambda j, *scalars: (j,) + (0,) * len(shape))


def fixed(shape):
    return pl.BlockSpec(shape, lambda j, *scalars: (0,) * len(shape))


gain_spec = pl.BlockSpec((1, GW), lambda j, member, *scalars: (0, member[0]))
t_spec = pl.BlockSpec((8, HD), lambda j, *scalars: (2 * COMP // 8, 0))


def over_members(kernel, scalars, in_specs, out_specs, out_shape, scratch, flops):
    return pl.pallas_call(
        kernel,
        out_shape=out_shape,
        grid_spec=pltpu.PrefetchScalarGridSpec(
            num_scalar_prefetch=scalars,
            grid=(KV,),
            in_specs=in_specs,
            out_specs=out_specs,
            scratch_shapes=scratch,
        ),
        compiler_params=pltpu.CompilerParams(dimension_semantics=("arbitrary",)),
        cost_estimate=pl.CostEstimate(flops=flops, transcendentals=0, bytes_accessed=4 << 20),
        interpret=INTERPRET,
    )


def shaped(shape, dtype):
    return jax.ShapeDtypeStruct(shape, dtype)


def section_tick(
    arriving,
    saved_input,
    returning,
    prompt_cache,
    fresh_cache,
    back_cache,
    query_gain,
    block_tables,
    fresh_lengths,
    back_lengths,
):
    member = (2 * lax.axis_index("fork_1") + lax.axis_index("fork_2")).astype(jnp.int32)[None]
    table = block_tables[0]
    keys = PROMPT + COMP
    four = range(KV)

    first = whole(
        pack_first_kernel, [shaped((FIRST_ROWS, HD), bf16)] * KV, [smem, vmem, vmem]
    )(member, prompt_cache[0], fresh_cache[0, 0])
    first = exchanged(first)
    incoming = whole(
        pack_arriving_kernel, [shaped((COMP, ARRIVE_W), bf16)] * KV, [smem, smem, vmem]
    )(member, fresh_lengths, arriving[0, 0])
    incoming = shifted_to_group(incoming, 1)
    slab = jnp.stack([part[0:HD] for part in first])
    slabs = jnp.broadcast_to(slab[None], (8, KV, HD, HD))
    pool = to_all(slabs, "fork_0").reshape(32, HD, HD)

    saved = whole(
        pack_saved_kernel, [shaped((COMP, SAVED_W), bf16)] * KV, [smem, smem, vmem, vmem]
    )(member, back_lengths, saved_input[0, 0], back_cache[0, 0])
    saved = exchanged(saved)
    cotangent = whole(
        pack_returning_kernel, [shaped((COMP, GW), bf16)] * KV, [smem, vmem]
    )(member, returning[0, 0])
    cotangent = shifted_to_group(cotangent, -1)

    *output, prompt_k, prompt_v = over_members(
        forward_kernel,
        2,
        [fixed((32, HD, HD))]
        + [fixed((COMP, ARRIVE_W)) for _ in four]
        + [fixed((FIRST_ROWS, HD)) for _ in four]
        + [gain_spec],
        [fixed((COMP, GW)) for _ in four] + [fixed((PROMPT, HD)), fixed((PROMPT, HD))],
        [shaped((COMP, GW), bf16) for _ in four]
        + [shaped((PROMPT, HD), bf16), shaped((PROMPT, HD), bf16)],
        [
            pltpu.VMEM((COMP, ARRIVE_W), bf16),
            pltpu.VMEM((FIRST_ROWS, HD), bf16),
            pltpu.VMEM((keys, HD), bf16),
            pltpu.VMEM((HD, keys), bf16),
            pltpu.VMEM((keys, 2 * COMP), f32),
            pltpu.VMEM((COMP, GW), bf16),
        ],
        4 * 4096 * keys * HD,
    )(member, table, pool, *incoming, *first, query_gain)
    output = exchanged(output)

    d_query, *own, reduced = over_members(
        backward_kernel,
        2,
        [fixed((COMP, SAVED_W)) for _ in four]
        + [fixed((COMP, GW)) for _ in four]
        + [fixed((PROMPT, HD)), fixed((PROMPT, HD)), gain_spec],
        [by_member((COMP, GW))]
        + [fixed((2 * COMP + 8, HD)) for _ in four]
        + [fixed((32, 144, HD))],
        [shaped((KV, COMP, GW), f32)]
        + [shaped((2 * COMP + 8, HD), f32) for _ in four]
        + [shaped((32, 144, HD), bf16)],
        [
            pltpu.VMEM((COMP, SAVED_W), bf16),
            pltpu.VMEM((COMP, GW), bf16),
            pltpu.VMEM((keys, HD), bf16),
            pltpu.VMEM((HD, keys), bf16),
            pltpu.VMEM((keys, HD), bf16),
            pltpu.VMEM((keys, HD), f32),
            pltpu.VMEM((keys, HD), f32),
            pltpu.VMEM((keys, 2 * COMP), f32),
            pltpu.VMEM((keys, 2 * COMP), f32),
            pltpu.VMEM((HEADS, HD), f32),
            pltpu.VMEM((32, HD), f32),
        ],
        10 * 4096 * keys * HD,
    )(member, table, *saved, *cotangent, prompt_k, prompt_v, query_gain)

    reduced = to_all(reduced, FORK)
    own = exchanged(own)

    input_grad = over_members(
        input_grad_kernel,
        1,
        [by_member((COMP, GW))]
        + [fixed((COMP, SAVED_W)) for _ in four]
        + [fixed((COMP, GW)) for _ in four]
        + [gain_spec]
        + [t_spec for _ in four],
        [fixed((COMP, GW)) for _ in four],
        [shaped((COMP, GW), bf16) for _ in four],
        [
            pltpu.VMEM((COMP, GW), bf16),
            pltpu.VMEM((COMP, SAVED_W), bf16),
            pltpu.VMEM((COMP, GW), bf16),
        ],
        1 << 20,
    )(member, d_query, *saved, *cotangent, query_gain, *own)
    input_grad = exchanged(input_grad)

    prompt_grad, gain_grad = whole(
        pool_sum_kernel, [shaped((2, 64, KV * HD), f32), shaped((KV, HEADS, HD), f32)], [vmem]
    )(reduced)

    joined = [smem] + [vmem] * KV
    rows = shaped((COMP, KV * GW), bf16)
    own_grad = whole(join_own_kernel, shaped((2, COMP, KV * HD), f32), joined)(member, *own)
    output = whole(join_rows_kernel, rows, joined)(member, *output)
    input_grad = whole(join_rows_kernel, rows, joined)(member, *input_grad)
    return (
        output[None, None],
        input_grad[None, None],
        prompt_grad[None],
        own_grad[None, None],
        gain_grad.reshape(1, KV * GW),
    )


def solution(mesh):
    finer = Mesh(
        mesh.devices.reshape(mesh.shape["section"], 8, 2, 2),
        ("section", "fork_0", "fork_1", "fork_2"),
    )
    placed = (
        P("section", FORK, None, None),
        P("section", FORK, None, None),
        P("section", FORK, None, None),
        P("section", None, FORK, None),
        P("section", FORK, None, None, None),
        P("section", FORK, None, None, None),
        P("section", None),
        P(FORK, None),
        P(FORK),
        P(FORK),
    )
    return jax.shard_map(
        section_tick,
        mesh=finer,
        in_specs=placed,
        out_specs=(
            P("section", FORK, None, None),
            P("section", FORK, None, None),
            P("section", None, FORK, None),
            P("section", FORK, None, None, None),
            P("section", None),
        ),
        check_vma=False,
    )
```

```python
import jax
import jax.numpy as jnp
from jax import lax
from jax.experimental import pallas as pl
from jax.experimental.pallas import tpu as pltpu
from jax.sharding import Mesh
from jax.sharding import PartitionSpec as P

KV = 4
HD = 128
BLOCK = 16
COMP = 128
NB = 64
GW = 1024
HEADS = 8
PROMPT = NB * BLOCK
SCALE = HD ** (-0.5)
FORK = ("fork_0", "fork_1", "fork_2")
QUAD = ("fork_1", "fork_2")
INTERPRET = False


epsilon = 1e-06
masked_score = -1e30
bf16 = jnp.bfloat16
f32 = jnp.float32

NT = (((1,), (1,)), ((), ()))

OWN_K, OWN_V, STATS = 1024, 1152, 1280
SAVED_W = 1408
ARRIVE_W = 1152
FIRST_ROWS = 384


def nt_dot(a, b):
    return lax.dot_general(a, b, NT, preferred_element_type=f32)


def nn_dot(a, b):
    return jnp.dot(a, b, preferred_element_type=f32)


def stats_tile(x, length):
    floated = x.astype(f32)
    inverse = lax.rsqrt(jnp.mean(floated * floated, axis=-1, keepdims=True) + epsilon)
    high = inverse.astype(bf16).astype(f32)
    rest = inverse - high
    middle = rest.astype(bf16).astype(f32)
    low = rest - middle
    lane = lax.broadcasted_iota(jnp.int32, (x.shape[0], HD), 1)
    tile = jnp.where(lane == 0, high, jnp.where(lane == 1, middle, jnp.where(lane == 2, low, 0.0)))
    tile = jnp.where(lane == 3, length.astype(f32), tile)
    return tile.astype(bf16)


def read_stats(tile):
    t = tile.astype(f32)
    inverse = t[:, 0:1] + t[:, 1:2] + t[:, 2:3]
    return inverse, t[:, 3:4]


def group_at(member, r, width):
    return pl.ds(pl.multiple_of(jnp.bitwise_xor(member[0], r) * width, width), width)


def pack_first_kernel(member, pool_ref, fresh_ref, *out_refs):
    for r in range(KV):
        cols = group_at(member, r, HD)
        out_refs[r][0:64, :] = pool_ref[0, :, cols]
        out_refs[r][64:128, :] = pool_ref[1, :, cols]
        out_refs[r][128:256, :] = fresh_ref[0, :, cols]
        out_refs[r][256:384, :] = fresh_ref[1, :, cols]


def pack_saved_kernel(member, length, x_ref, back_ref, *out_refs):
    tile = stats_tile(x_ref[...], length[0])
    for r in range(KV):
        out_ref = out_refs[r]
        out_ref[:, 0:GW] = x_ref[:, group_at(member, r, GW)]
        cols = group_at(member, r, HD)
        out_ref[:, OWN_K : OWN_K + HD] = back_ref[0, :, cols]
        out_ref[:, OWN_V : OWN_V + HD] = back_ref[1, :, cols]
        out_ref[:, STATS : STATS + HD] = tile


def pack_returning_kernel(member, x_ref, *out_refs):
    for r in range(KV):
        out_refs[r][...] = x_ref[:, group_at(member, r, GW)]


def pack_arriving_kernel(member, length, x_ref, *out_refs):
    tile = stats_tile(x_ref[...], length[0])
    for r in range(KV):
        out_refs[r][:, 0:GW] = x_ref[:, group_at(member, r, GW)]
        out_refs[r][:, GW : GW + HD] = tile


TOGETHER = 4
COLS = TOGETHER * COMP
STEP = 64
NKEYS = PROMPT + COMP
NSTEP = NKEYS // STEP
LOG2E = 1.4426950408889634


def some_heads(rows, part):
    a = part * TOGETHER * HD
    return jnp.concatenate([rows[:, a + e * HD : a + (e + 1) * HD] for e in range(TOGETHER)], axis=0)


def own_mask(length):
    u = lax.broadcasted_iota(jnp.int32, (COMP, COLS), 0)
    i = lax.broadcasted_iota(jnp.int32, (COMP, COLS), 1) & (COMP - 1)
    return (u <= i) & (u.astype(f32) < length[0:1, 0:1])


def steps():
    return [slice(c * STEP, (c + 1) * STEP) for c in range(NSTEP)]


def softmax_columns(s_ref, mask):
    s_ref[PROMPT:, :] = jnp.where(mask, s_ref[PROMPT:, :], masked_score)
    top = None
    for rows in steps():
        part = jnp.max(s_ref[rows, :], axis=0, keepdims=True)
        top = part if top is None else jnp.maximum(top, part)
    top = top * (SCALE * LOG2E)
    total = None
    for rows in steps():
        p = jnp.exp2(s_ref[rows, :] * (SCALE * LOG2E) - top)
        s_ref[rows, :] = p
        part = jnp.sum(p, axis=0, keepdims=True)
        total = part if total is None else total + part
    return 1.0 / total


def put_by_step(j, out_refs, from_ref):
    for r in range(KV):

        @pl.when(j == r)
        def _(r=r):
            out_refs[r][...] = from_ref[...]


def take_by_step(j, from_refs, to_ref):
    for r in range(KV):

        @pl.when(j == r)
        def _(r=r):
            to_ref[...] = from_refs[r][...]


def backward_kernel(
    member, table, saved_0, saved_1, saved_2, saved_3, grad_0, grad_1, grad_2, grad_3,
    prompt_k_ref, prompt_v_ref, gain_ref,
    dq_ref, own_0, own_1, own_2, own_3, reduce_ref, t_ref,
    saved_ref, grad_ref,
    keys_ref, keys_t_ref, values_ref, dk_ref, dv_ref, s_refs, w_refs, b_refs, gain_acc,
):
    j = pl.program_id(0)
    own_refs = (own_0, own_1, own_2, own_3)
    take_by_step(j, (saved_0, saved_1, saved_2, saved_3), saved_ref)
    take_by_step(j, (grad_0, grad_1, grad_2, grad_3), grad_ref)

    @pl.when(j == 0)
    def _():
        keys_ref[0:PROMPT, :] = prompt_k_ref[...]
        values_ref[0:PROMPT, :] = prompt_v_ref[...]
        for c in range(PROMPT // HD):
            rows = slice(c * HD, (c + 1) * HD)
            keys_t_ref[:, rows] = keys_ref[rows, :].astype(f32).T.astype(bf16)
        dk_ref[0:PROMPT, :] = jnp.zeros((PROMPT, HD), f32)
        dv_ref[0:PROMPT, :] = jnp.zeros((PROMPT, HD), f32)
        gain_acc[...] = jnp.zeros(gain_acc.shape, f32)

    inverse, length = read_stats(saved_ref[:, STATS : STATS + HD])
    x = saved_ref[:, 0:GW].astype(f32)
    normal = x * inverse
    gain = gain_ref[...]
    q = (normal * gain).astype(bf16)
    row = lax.broadcasted_iota(jnp.int32, (COMP, 1), 0).astype(f32)
    valid = row < length
    d_out = jnp.where(valid, grad_ref[...].astype(f32), 0.0).astype(bf16)
    keys_ref[PROMPT:, :] = saved_ref[:, OWN_K : OWN_K + HD]
    values_ref[PROMPT:, :] = saved_ref[:, OWN_V : OWN_V + HD]
    keys_t_ref[:, PROMPT:] = saved_ref[:, OWN_K : OWN_K + HD].astype(f32).T.astype(bf16)
    dk_ref[PROMPT:, :] = jnp.zeros((COMP, HD), f32)
    dv_ref[PROMPT:, :] = jnp.zeros((COMP, HD), f32)
    mask = own_mask(length)

    t = jnp.zeros((COMP, 1), f32)
    for part in range(HEADS // TOGETHER):
        s_refs[part, :, :] = nt_dot(keys_ref[...], some_heads(q, part))
        w_refs[part, :, :] = nt_dot(values_ref[...], some_heads(d_out, part))
    for part in range(HEADS // TOGETHER):
        q_rows = some_heads(q, part)
        d_rows = some_heads(d_out, part)
        s_ref, w_ref, b_ref = s_refs.at[part], w_refs.at[part], b_refs.at[part]
        ratio = softmax_columns(s_ref, mask)
        delta = None
        for rows in steps():
            a = s_ref[rows, :] * ratio
            s_ref[rows, :] = a
            b_ref[rows, :] = a.astype(bf16)
            piece = jnp.sum(a * w_ref[rows, :], axis=0, keepdims=True)
            delta = piece if delta is None else delta + piece
        dv_ref[...] += nn_dot(b_ref[...], d_rows)
        for rows in steps():
            b_ref[rows, :] = (s_ref[rows, :] * (w_ref[rows, :] - delta) * SCALE).astype(bf16)
        dk_ref[...] += nn_dot(b_ref[...], q_rows)
        dq_t = nn_dot(keys_t_ref[...], b_ref[...])
        for e in range(TOGETHER):
            h = TOGETHER * part + e
            cols = slice(h * HD, (h + 1) * HD)
            dq = dq_t[:, e * HD : (e + 1) * HD].T
            dq_ref[0, :, cols] = dq
            t = t + jnp.sum(dq * gain[:, cols] * x[:, cols], axis=1, keepdims=True)
            gain_acc[h : h + 1, :] += jnp.sum(dq * normal[:, cols], axis=0, keepdims=True)

    for r in range(KV):

        @pl.when(j == r)
        def _(r=r):
            own_refs[r][0:COMP, :] = dk_ref[PROMPT:, :]
            own_refs[r][COMP : 2 * COMP, :] = dv_ref[PROMPT:, :]

    @pl.when(j == 0)
    def _():
        t_ref[...] = jnp.zeros((8, HD), f32)

    place = lax.broadcasted_iota(jnp.int32, (8, HD), 0)
    t_rows = jnp.broadcast_to(t, (COMP, HD)).T[0:8, :]
    t_ref[...] = jnp.where(place == jnp.bitwise_xor(j, member[0]), t_rows, t_ref[...])

    @pl.when(j == KV - 1)
    def _():
        high = gain_acc[...].astype(bf16)
        low = (gain_acc[...] - high.astype(f32)).astype(bf16)
        both = jnp.concatenate([high, low], axis=0)

        def clear(n, carry):
            reduce_ref[n, 0:HD, :] = jnp.zeros((HD, HD), bf16)
            reduce_ref[n, HD : HD + 16, :] = both
            return carry

        lax.fori_loop(0, 32, clear, 0)

        def spread(n, carry):
            b = table[n]
            holder = b // 4
            at = pl.multiple_of((b % 4) * BLOCK, BLOCK)
            start = pl.multiple_of(n * BLOCK, BLOCK)
            reduce_ref[holder, pl.ds(at, BLOCK), :] = dk_ref[pl.ds(start, BLOCK), :].astype(bf16)
            reduce_ref[holder, pl.ds(at + 64, BLOCK), :] = dv_ref[pl.ds(start, BLOCK), :].astype(bf16)
            return carry

        lax.fori_loop(0, NB, spread, 0)


def forward_kernel(
    member, table, pool_ref, arrive_0, arrive_1, arrive_2, arrive_3,
    first_0, first_1, first_2, first_3, gain_ref,
    out_0, out_1, out_2, out_3, prompt_k_ref, prompt_v_ref,
    arrive_ref, first_ref, keys_ref, values_t_ref, s_refs, b_refs, y_ref,
):
    j = pl.program_id(0)
    take_by_step(j, (arrive_0, arrive_1, arrive_2, arrive_3), arrive_ref)
    take_by_step(j, (first_0, first_1, first_2, first_3), first_ref)

    @pl.when(j == 0)
    def _():
        def pick(n, carry):
            b = table[n]
            place = (b // 16) * KV + jnp.bitwise_xor((b // 4) % 4, member[0])
            at = pl.multiple_of((b % 4) * BLOCK, BLOCK)
            to = pl.multiple_of(n * BLOCK, BLOCK)
            prompt_k_ref[pl.ds(to, BLOCK), :] = pool_ref[place, pl.ds(at, BLOCK), :]
            prompt_v_ref[pl.ds(to, BLOCK), :] = pool_ref[place, pl.ds(at + 64, BLOCK), :]
            return carry

        lax.fori_loop(0, NB, pick, 0)
        keys_ref[0:PROMPT, :] = prompt_k_ref[...]
        for c in range(PROMPT // HD):
            rows = slice(c * HD, (c + 1) * HD)
            values_t_ref[:, rows] = prompt_v_ref[rows, :].astype(f32).T.astype(bf16)

    inverse, length = read_stats(arrive_ref[:, GW : GW + HD])
    x = arrive_ref[:, 0:GW].astype(f32)
    q = (x * inverse * gain_ref[...]).astype(bf16)
    row = lax.broadcasted_iota(jnp.int32, (COMP, 1), 0).astype(f32)
    valid = row < length
    keys_ref[PROMPT:, :] = first_ref[128:256, :]
    values_t_ref[:, PROMPT:] = first_ref[256:384, :].astype(f32).T.astype(bf16)
    mask = own_mask(length)
    for part in range(HEADS // TOGETHER):
        s_refs[part, :, :] = nt_dot(keys_ref[...], some_heads(q, part))
    for part in range(HEADS // TOGETHER):
        s_ref, b_ref = s_refs.at[part], b_refs.at[part]
        ratio = softmax_columns(s_ref, mask)
        for rows in steps():
            b_ref[rows, :] = (s_ref[rows, :] * ratio).astype(bf16)
        o_t = nn_dot(values_t_ref[...], b_ref[...])
        for e in range(TOGETHER):
            h = TOGETHER * part + e
            cols = slice(h * HD, (h + 1) * HD)
            o = jnp.where(valid, o_t[:, e * HD : (e + 1) * HD].T, 0.0)
            y_ref[:, cols] = (x[:, cols] + o).astype(bf16)
    put_by_step(j, (out_0, out_1, out_2, out_3), y_ref)


def input_grad_kernel(
    member, dq_ref, saved_0, saved_1, saved_2, saved_3, grad_0, grad_1, grad_2, grad_3,
    gain_ref, t_0, t_1, t_2, t_3, out_0, out_1, out_2, out_3, y_ref, saved_ref, grad_ref
):
    j = pl.program_id(0)
    take_by_step(j, (saved_0, saved_1, saved_2, saved_3), saved_ref)
    take_by_step(j, (grad_0, grad_1, grad_2, grad_3), grad_ref)
    inverse, _ = read_stats(saved_ref[:, STATS : STATS + HD])
    total = t_0[...] + t_1[...] + t_2[...] + t_3[...]
    place = lax.broadcasted_iota(jnp.int32, (8, HD), 0)
    t_row = jnp.sum(jnp.where(place == jnp.bitwise_xor(j, member[0]), total, 0.0), axis=0, keepdims=True)
    t = jnp.broadcast_to(t_row, (HD, HD)).T[:, 0:1] * (1.0 / (KV * GW))
    x = saved_ref[:, 0:GW].astype(f32)
    dx = inverse * (dq_ref[0] * gain_ref[...]) - x * (inverse * inverse * inverse * t)
    y_ref[...] = (grad_ref[...].astype(f32) + dx).astype(bf16)
    put_by_step(j, (out_0, out_1, out_2, out_3), y_ref)


def pool_sum_kernel(got_ref, out_ref, gain_ref):
    for g in range(KV):
        total = got_ref[g].astype(f32)
        for z in range(1, 8):
            total = total + got_ref[z * KV + g].astype(f32)
        cols = slice(g * HD, (g + 1) * HD)
        out_ref[0, :, cols] = total[0:64, :]
        out_ref[1, :, cols] = total[64:128, :]
        gain_ref[g] = total[128:136, :] + total[136:144, :]


def join_rows_kernel(member, *refs):
    out_ref = refs[KV]
    for r in range(KV):
        out_ref[:, group_at(member, r, GW)] = refs[r][...]


def join_own_kernel(member, *refs):
    out_ref = refs[KV]
    for r in range(KV):
        cols = group_at(member, r, HD)
        out_ref[0, :, cols] = refs[r][0:COMP, :]
        out_ref[1, :, cols] = refs[r][COMP : 2 * COMP, :]


smem = pl.BlockSpec(memory_space=pltpu.SMEM)
vmem = pl.BlockSpec(memory_space=pltpu.VMEM)


def whole(kernel, out_shape, in_specs):
    count = len(out_shape) if isinstance(out_shape, (list, tuple)) else None
    return pl.pallas_call(
        kernel,
        out_shape=out_shape,
        in_specs=in_specs,
        out_specs=[vmem] * count if count else vmem,
        interpret=INTERPRET,
    )


def shifted_to_group(values, steps):
    sections = lax.axis_size("section")
    got = []
    for r, value in enumerate(values):
        pairs = [
            (s * KV + k, ((s + steps) % sections) * KV + (k ^ r))
            for s in range(sections)
            for k in range(KV)
        ]
        got.append(lax.ppermute(value, ("section",) + QUAD, pairs))
    return got


def exchanged(values):
    pairs = lambda r: [(k, k ^ r) for k in range(KV)]
    return [values[0]] + [lax.ppermute(values[r], QUAD, pairs(r)) for r in range(1, KV)]


def to_all(tiles, axes):
    return lax.all_to_all(tiles, axes, 0, 0, tiled=True)


def by_member(shape):
    return pl.BlockSpec((1,) + shape, lambda j, *scalars: (j,) + (0,) * len(shape))


def fixed(shape):
    return pl.BlockSpec(shape, lambda j, *scalars: (0,) * len(shape))


gain_spec = pl.BlockSpec((1, GW), lambda j, member, *scalars: (0, member[0]))


def over_members(kernel, scalars, in_specs, out_specs, out_shape, scratch, flops):
    return pl.pallas_call(
        kernel,
        out_shape=out_shape,
        grid_spec=pltpu.PrefetchScalarGridSpec(
            num_scalar_prefetch=scalars,
            grid=(KV,),
            in_specs=in_specs,
            out_specs=out_specs,
            scratch_shapes=scratch,
        ),
        compiler_params=pltpu.CompilerParams(dimension_semantics=("arbitrary",)),
        cost_estimate=pl.CostEstimate(flops=flops, transcendentals=0, bytes_accessed=4 << 20),
        interpret=INTERPRET,
    )


def shaped(shape, dtype):
    return jax.ShapeDtypeStruct(shape, dtype)


def section_tick(
    arriving,
    saved_input,
    returning,
    prompt_cache,
    fresh_cache,
    back_cache,
    query_gain,
    block_tables,
    fresh_lengths,
    back_lengths,
):
    member = (2 * lax.axis_index("fork_1") + lax.axis_index("fork_2")).astype(jnp.int32)[None]
    table = block_tables[0]
    keys = PROMPT + COMP
    four = range(KV)

    first = whole(
        pack_first_kernel, [shaped((FIRST_ROWS, HD), bf16)] * KV, [smem, vmem, vmem]
    )(member, prompt_cache[0], fresh_cache[0, 0])
    first = exchanged(first)
    incoming = whole(
        pack_arriving_kernel, [shaped((COMP, ARRIVE_W), bf16)] * KV, [smem, smem, vmem]
    )(member, fresh_lengths, arriving[0, 0])
    incoming = shifted_to_group(incoming, 1)
    slab = jnp.stack([part[0:HD] for part in first])
    slabs = jnp.broadcast_to(slab[None], (8, KV, HD, HD))
    pool = to_all(slabs, "fork_0").reshape(32, HD, HD)

    saved = whole(
        pack_saved_kernel, [shaped((COMP, SAVED_W), bf16)] * KV, [smem, smem, vmem, vmem]
    )(member, back_lengths, saved_input[0, 0], back_cache[0, 0])
    saved = exchanged(saved)
    cotangent = whole(
        pack_returning_kernel, [shaped((COMP, GW), bf16)] * KV, [smem, vmem]
    )(member, returning[0, 0])
    cotangent = shifted_to_group(cotangent, -1)

    *output, prompt_k, prompt_v = over_members(
        forward_kernel,
        2,
        [fixed((32, HD, HD))]
        + [fixed((COMP, ARRIVE_W)) for _ in four]
        + [fixed((FIRST_ROWS, HD)) for _ in four]
        + [gain_spec],
        [fixed((COMP, GW)) for _ in four] + [fixed((PROMPT, HD)), fixed((PROMPT, HD))],
        [shaped((COMP, GW), bf16) for _ in four]
        + [shaped((PROMPT, HD), bf16), shaped((PROMPT, HD), bf16)],
        [
            pltpu.VMEM((COMP, ARRIVE_W), bf16),
            pltpu.VMEM((FIRST_ROWS, HD), bf16),
            pltpu.VMEM((keys, HD), bf16),
            pltpu.VMEM((HD, keys), bf16),
            pltpu.VMEM((HEADS // TOGETHER, keys, COLS), f32),
            pltpu.VMEM((HEADS // TOGETHER, keys, COLS), bf16),
            pltpu.VMEM((COMP, GW), bf16),
        ],
        4 * 4096 * keys * HD,
    )(member, table, pool, *incoming, *first, query_gain)
    output = exchanged(output)

    d_query, *own, reduced, t_part = over_members(
        backward_kernel,
        2,
        [fixed((COMP, SAVED_W)) for _ in four]
        + [fixed((COMP, GW)) for _ in four]
        + [fixed((PROMPT, HD)), fixed((PROMPT, HD)), gain_spec],
        [by_member((COMP, GW))]
        + [fixed((2 * COMP, HD)) for _ in four]
        + [fixed((32, 144, HD)), fixed((8, HD))],
        [shaped((KV, COMP, GW), f32)]
        + [shaped((2 * COMP, HD), f32) for _ in four]
        + [shaped((32, 144, HD), bf16), shaped((8, HD), f32)],
        [
            pltpu.VMEM((COMP, SAVED_W), bf16),
            pltpu.VMEM((COMP, GW), bf16),
            pltpu.VMEM((keys, HD), bf16),
            pltpu.VMEM((HD, keys), bf16),
            pltpu.VMEM((keys, HD), bf16),
            pltpu.VMEM((keys, HD), f32),
            pltpu.VMEM((keys, HD), f32),
            pltpu.VMEM((HEADS // TOGETHER, keys, COLS), f32),
            pltpu.VMEM((HEADS // TOGETHER, keys, COLS), f32),
            pltpu.VMEM((HEADS // TOGETHER, keys, COLS), bf16),
            pltpu.VMEM((HEADS, HD), f32),
        ],
        10 * 4096 * keys * HD,
    )(member, table, *saved, *cotangent, prompt_k, prompt_v, query_gain)

    t_parts = exchanged([t_part] * KV)
    reduced = to_all(reduced, FORK)
    own = exchanged(own)

    input_grad = over_members(
        input_grad_kernel,
        1,
        [by_member((COMP, GW))]
        + [fixed((COMP, SAVED_W)) for _ in four]
        + [fixed((COMP, GW)) for _ in four]
        + [gain_spec]
        + [fixed((8, HD)) for _ in four],
        [fixed((COMP, GW)) for _ in four],
        [shaped((COMP, GW), bf16) for _ in four],
        [
            pltpu.VMEM((COMP, GW), bf16),
            pltpu.VMEM((COMP, SAVED_W), bf16),
            pltpu.VMEM((COMP, GW), bf16),
        ],
        1 << 20,
    )(member, d_query, *saved, *cotangent, query_gain, *t_parts)
    input_grad = exchanged(input_grad)

    prompt_grad, gain_grad = whole(
        pool_sum_kernel, [shaped((2, 64, KV * HD), f32), shaped((KV, HEADS, HD), f32)], [vmem]
    )(reduced)

    joined = [smem] + [vmem] * KV
    rows = shaped((COMP, KV * GW), bf16)
    own_grad = whole(join_own_kernel, shaped((2, COMP, KV * HD), f32), joined)(member, *own)
    output = whole(join_rows_kernel, rows, joined)(member, *output)
    input_grad = whole(join_rows_kernel, rows, joined)(member, *input_grad)
    return (
        output[None, None],
        input_grad[None, None],
        prompt_grad[None],
        own_grad[None, None],
        gain_grad.reshape(1, KV * GW),
    )


def solution(mesh):
    finer = Mesh(
        mesh.devices.reshape(mesh.shape["section"], 8, 2, 2),
        ("section", "fork_0", "fork_1", "fork_2"),
    )
    placed = (
        P("section", FORK, None, None),
        P("section", FORK, None, None),
        P("section", FORK, None, None),
        P("section", None, FORK, None),
        P("section", FORK, None, None, None),
        P("section", FORK, None, None, None),
        P("section", None),
        P(FORK, None),
        P(FORK),
        P(FORK),
    )
    return jax.shard_map(
        section_tick,
        mesh=finer,
        in_specs=placed,
        out_specs=(
            P("section", FORK, None, None),
            P("section", FORK, None, None),
            P("section", None, FORK, None),
            P("section", FORK, None, None, None),
            P("section", None),
        ),
        check_vma=False,
    )
```

```python
import jax
import jax.numpy as jnp
from jax import lax
from jax.experimental import pallas as pl
from jax.experimental.pallas import tpu as pltpu
from jax.sharding import Mesh
from jax.sharding import PartitionSpec as P

KV = 4
HD = 128
BLOCK = 16
COMP = 128
NB = 64
GW = 1024
HEADS = 8
PROMPT = NB * BLOCK
SCALE = HD ** (-0.5)
FORK = ("fork_0", "fork_1", "fork_2")
QUAD = ("fork_1", "fork_2")
INTERPRET = False


epsilon = 1e-06
masked_score = -1e30
bf16 = jnp.bfloat16
f32 = jnp.float32

NT = (((1,), (1,)), ((), ()))

OWN_K, OWN_V, STATS = 1024, 1152, 1280
SAVED_W = 1408
ARRIVE_W = 1152
FIRST_ROWS = 384


def nt_dot(a, b):
    return lax.dot_general(a, b, NT, preferred_element_type=f32)


def nn_dot(a, b):
    return jnp.dot(a, b, preferred_element_type=f32)


def stats_tile(x, length):
    floated = x.astype(f32)
    inverse = lax.rsqrt(jnp.mean(floated * floated, axis=-1, keepdims=True) + epsilon)
    high = inverse.astype(bf16).astype(f32)
    rest = inverse - high
    middle = rest.astype(bf16).astype(f32)
    low = rest - middle
    lane = lax.broadcasted_iota(jnp.int32, (x.shape[0], HD), 1)
    tile = jnp.where(lane == 0, high, jnp.where(lane == 1, middle, jnp.where(lane == 2, low, 0.0)))
    tile = jnp.where(lane == 3, length.astype(f32), tile)
    return tile.astype(bf16)


def read_stats(tile):
    t = tile.astype(f32)
    inverse = t[:, 0:1] + t[:, 1:2] + t[:, 2:3]
    return inverse, t[:, 3:4]


def group_at(member, r, width):
    return pl.ds(pl.multiple_of(jnp.bitwise_xor(member[0], r) * width, width), width)


def pack_first_kernel(member, pool_ref, fresh_ref, *out_refs):
    for r in range(KV):
        cols = group_at(member, r, HD)
        out_refs[r][0:64, :] = pool_ref[0, :, cols]
        out_refs[r][64:128, :] = pool_ref[1, :, cols]
        out_refs[r][128:256, :] = fresh_ref[0, :, cols]
        out_refs[r][256:384, :] = fresh_ref[1, :, cols]


def pack_saved_kernel(member, length, x_ref, back_ref, *out_refs):
    tile = stats_tile(x_ref[...], length[0])
    for r in range(KV):
        out_ref = out_refs[r]
        out_ref[:, 0:GW] = x_ref[:, group_at(member, r, GW)]
        cols = group_at(member, r, HD)
        out_ref[:, OWN_K : OWN_K + HD] = back_ref[0, :, cols]
        out_ref[:, OWN_V : OWN_V + HD] = back_ref[1, :, cols]
        out_ref[:, STATS : STATS + HD] = tile


def pack_returning_kernel(member, x_ref, *out_refs):
    for r in range(KV):
        out_refs[r][...] = x_ref[:, group_at(member, r, GW)]


def pack_arriving_kernel(member, length, x_ref, *out_refs):
    tile = stats_tile(x_ref[...], length[0])
    for r in range(KV):
        out_refs[r][:, 0:GW] = x_ref[:, group_at(member, r, GW)]
        out_refs[r][:, GW : GW + HD] = tile


TOGETHER = 4
COLS = TOGETHER * COMP
STEP = 64
NKEYS = PROMPT + COMP
NSTEP = NKEYS // STEP
LOG2E = 1.4426950408889634


def some_heads(rows, part):
    a = part * TOGETHER * HD
    return jnp.concatenate([rows[:, a + e * HD : a + (e + 1) * HD] for e in range(TOGETHER)], axis=0)


def own_mask(length):
    u = lax.broadcasted_iota(jnp.int32, (COMP, COLS), 0)
    i = lax.broadcasted_iota(jnp.int32, (COMP, COLS), 1) & (COMP - 1)
    return (u <= i) & (u.astype(f32) < length[0:1, 0:1])


def steps():
    return [slice(c * STEP, (c + 1) * STEP) for c in range(NSTEP)]


def softmax_columns(s_ref, mask):
    s_ref[PROMPT:, :] = jnp.where(mask, s_ref[PROMPT:, :], masked_score)
    top = None
    for rows in steps():
        part = jnp.max(s_ref[rows, :], axis=0, keepdims=True)
        top = part if top is None else jnp.maximum(top, part)
    top = top * (SCALE * LOG2E)
    total = None
    for rows in steps():
        p = jnp.exp2(s_ref[rows, :] * (SCALE * LOG2E) - top)
        s_ref[rows, :] = p
        part = jnp.sum(p, axis=0, keepdims=True)
        total = part if total is None else total + part
    return 1.0 / total


def put_by_step(j, out_refs, from_ref):
    for r in range(KV):

        @pl.when(j == r)
        def _(r=r):
            out_refs[r][...] = from_ref[...]


def take_by_step(j, from_refs, to_ref):
    for r in range(KV):

        @pl.when(j == r)
        def _(r=r):
            to_ref[...] = from_refs[r][...]


def backward_kernel(
    member, table, saved_0, saved_1, saved_2, saved_3, grad_0, grad_1, grad_2, grad_3,
    prompt_k_ref, prompt_v_ref, gain_ref,
    dq_ref, own_0, own_1, own_2, own_3, reduce_ref,
    saved_ref, grad_ref,
    keys_ref, keys_t_ref, values_ref, dk_ref, dv_ref, s_refs, w_refs, b_refs, gain_acc, t_ref,
):
    j = pl.program_id(0)
    own_refs = (own_0, own_1, own_2, own_3)
    take_by_step(j, (saved_0, saved_1, saved_2, saved_3), saved_ref)
    take_by_step(j, (grad_0, grad_1, grad_2, grad_3), grad_ref)

    @pl.when(j == 0)
    def _():
        keys_ref[0:PROMPT, :] = prompt_k_ref[...]
        values_ref[0:PROMPT, :] = prompt_v_ref[...]
        for c in range(PROMPT // HD):
            rows = slice(c * HD, (c + 1) * HD)
            keys_t_ref[:, rows] = keys_ref[rows, :].astype(f32).T.astype(bf16)
        dk_ref[0:PROMPT, :] = jnp.zeros((PROMPT, HD), f32)
        dv_ref[0:PROMPT, :] = jnp.zeros((PROMPT, HD), f32)
        gain_acc[...] = jnp.zeros(gain_acc.shape, f32)

    inverse, length = read_stats(saved_ref[:, STATS : STATS + HD])
    x = saved_ref[:, 0:GW].astype(f32)
    normal = x * inverse
    gain = gain_ref[...]
    q = (normal * gain).astype(bf16)
    row = lax.broadcasted_iota(jnp.int32, (COMP, 1), 0).astype(f32)
    valid = row < length
    d_out = jnp.where(valid, grad_ref[...].astype(f32), 0.0).astype(bf16)
    keys_ref[PROMPT:, :] = saved_ref[:, OWN_K : OWN_K + HD]
    values_ref[PROMPT:, :] = saved_ref[:, OWN_V : OWN_V + HD]
    keys_t_ref[:, PROMPT:] = saved_ref[:, OWN_K : OWN_K + HD].astype(f32).T.astype(bf16)
    dk_ref[PROMPT:, :] = jnp.zeros((COMP, HD), f32)
    dv_ref[PROMPT:, :] = jnp.zeros((COMP, HD), f32)
    mask = own_mask(length)

    t = jnp.zeros((COMP, 1), f32)
    for part in range(HEADS // TOGETHER):
        s_refs[part, :, :] = nt_dot(keys_ref[...], some_heads(q, part))
        w_refs[part, :, :] = nt_dot(values_ref[...], some_heads(d_out, part))
    for part in range(HEADS // TOGETHER):
        q_rows = some_heads(q, part)
        d_rows = some_heads(d_out, part)
        s_ref, w_ref, b_ref = s_refs.at[part], w_refs.at[part], b_refs.at[part]
        ratio = softmax_columns(s_ref, mask)
        delta = None
        for rows in steps():
            a = s_ref[rows, :] * ratio
            s_ref[rows, :] = a
            b_ref[rows, :] = a.astype(bf16)
            piece = jnp.sum(a * w_ref[rows, :], axis=0, keepdims=True)
            delta = piece if delta is None else delta + piece
        dv_ref[...] += nn_dot(b_ref[...], d_rows)
        for rows in steps():
            b_ref[rows, :] = (s_ref[rows, :] * (w_ref[rows, :] - delta) * SCALE).astype(bf16)
        dk_ref[...] += nn_dot(b_ref[...], q_rows)
        dq_t = nn_dot(keys_t_ref[...], b_ref[...])
        for e in range(TOGETHER):
            h = TOGETHER * part + e
            cols = slice(h * HD, (h + 1) * HD)
            dq = dq_t[:, e * HD : (e + 1) * HD].T
            dq_ref[0, :, cols] = dq
            t = t + jnp.sum(dq * gain[:, cols] * x[:, cols], axis=1, keepdims=True)
            gain_acc[h : h + 1, :] += jnp.sum(dq * normal[:, cols], axis=0, keepdims=True)

    for r in range(KV):

        @pl.when(j == r)
        def _(r=r):
            own_refs[r][0:COMP, :] = dk_ref[PROMPT:, :]
            own_refs[r][COMP : 2 * COMP, :] = dv_ref[PROMPT:, :]

    @pl.when(j == 0)
    def _():
        t_ref[...] = jnp.zeros((8, HD), f32)

    place = lax.broadcasted_iota(jnp.int32, (8, HD), 0)
    t_rows = jnp.broadcast_to(t, (COMP, HD)).T[0:8, :]
    t_ref[...] = jnp.where(place == jnp.bitwise_xor(j, member[0]), t_rows, t_ref[...])

    @pl.when(j == KV - 1)
    def _():
        for own_ref in own_refs:
            own_ref[2 * COMP :, :] = t_ref[...]
        high = gain_acc[...].astype(bf16)
        low = (gain_acc[...] - high.astype(f32)).astype(bf16)
        both = jnp.concatenate([high, low], axis=0)

        def clear(n, carry):
            reduce_ref[n, 0:HD, :] = jnp.zeros((HD, HD), bf16)
            reduce_ref[n, HD : HD + 16, :] = both
            return carry

        lax.fori_loop(0, 32, clear, 0)

        def spread(n, carry):
            b = table[n]
            holder = b // 4
            at = pl.multiple_of((b % 4) * BLOCK, BLOCK)
            start = pl.multiple_of(n * BLOCK, BLOCK)
            reduce_ref[holder, pl.ds(at, BLOCK), :] = dk_ref[pl.ds(start, BLOCK), :].astype(bf16)
            reduce_ref[holder, pl.ds(at + 64, BLOCK), :] = dv_ref[pl.ds(start, BLOCK), :].astype(bf16)
            return carry

        lax.fori_loop(0, NB, spread, 0)


def forward_kernel(
    member, table, pool_ref, arrive_0, arrive_1, arrive_2, arrive_3,
    first_0, first_1, first_2, first_3, gain_ref,
    out_0, out_1, out_2, out_3, prompt_k_ref, prompt_v_ref,
    arrive_ref, first_ref, keys_ref, values_t_ref, s_refs, b_refs, y_ref,
):
    j = pl.program_id(0)
    take_by_step(j, (arrive_0, arrive_1, arrive_2, arrive_3), arrive_ref)
    take_by_step(j, (first_0, first_1, first_2, first_3), first_ref)

    @pl.when(j == 0)
    def _():
        def pick(n, carry):
            b = table[n]
            far = (member[1] - b // 16 + 8) % 8
            place = far * KV + jnp.bitwise_xor((b // 4) % 4, member[0])
            at = pl.multiple_of((b % 4) * BLOCK, BLOCK)
            to = pl.multiple_of(n * BLOCK, BLOCK)
            prompt_k_ref[pl.ds(to, BLOCK), :] = pool_ref[place, pl.ds(at, BLOCK), :]
            prompt_v_ref[pl.ds(to, BLOCK), :] = pool_ref[place, pl.ds(at + 64, BLOCK), :]
            return carry

        lax.fori_loop(0, NB, pick, 0)
        keys_ref[0:PROMPT, :] = prompt_k_ref[...]
        for c in range(PROMPT // HD):
            rows = slice(c * HD, (c + 1) * HD)
            values_t_ref[:, rows] = prompt_v_ref[rows, :].astype(f32).T.astype(bf16)

    inverse, length = read_stats(arrive_ref[:, GW : GW + HD])
    x = arrive_ref[:, 0:GW].astype(f32)
    q = (x * inverse * gain_ref[...]).astype(bf16)
    row = lax.broadcasted_iota(jnp.int32, (COMP, 1), 0).astype(f32)
    valid = row < length
    keys_ref[PROMPT:, :] = first_ref[128:256, :]
    values_t_ref[:, PROMPT:] = first_ref[256:384, :].astype(f32).T.astype(bf16)
    mask = own_mask(length)
    for part in range(HEADS // TOGETHER):
        s_refs[part, :, :] = nt_dot(keys_ref[...], some_heads(q, part))
    for part in range(HEADS // TOGETHER):
        s_ref, b_ref = s_refs.at[part], b_refs.at[part]
        ratio = softmax_columns(s_ref, mask)
        for rows in steps():
            b_ref[rows, :] = (s_ref[rows, :] * ratio).astype(bf16)
        o_t = nn_dot(values_t_ref[...], b_ref[...])
        for e in range(TOGETHER):
            h = TOGETHER * part + e
            cols = slice(h * HD, (h + 1) * HD)
            o = jnp.where(valid, o_t[:, e * HD : (e + 1) * HD].T, 0.0)
            y_ref[:, cols] = (x[:, cols] + o).astype(bf16)
    put_by_step(j, (out_0, out_1, out_2, out_3), y_ref)


def input_grad_kernel(
    member, dq_ref, saved_0, saved_1, saved_2, saved_3, grad_0, grad_1, grad_2, grad_3,
    gain_ref, t_0, t_1, t_2, t_3, out_0, out_1, out_2, out_3, y_ref, saved_ref, grad_ref
):
    j = pl.program_id(0)
    take_by_step(j, (saved_0, saved_1, saved_2, saved_3), saved_ref)
    take_by_step(j, (grad_0, grad_1, grad_2, grad_3), grad_ref)
    inverse, _ = read_stats(saved_ref[:, STATS : STATS + HD])
    total = t_0[...] + t_1[...] + t_2[...] + t_3[...]
    place = lax.broadcasted_iota(jnp.int32, (8, HD), 0)
    t_row = jnp.sum(jnp.where(place == jnp.bitwise_xor(j, member[0]), total, 0.0), axis=0, keepdims=True)
    t = jnp.broadcast_to(t_row, (HD, HD)).T[:, 0:1] * (1.0 / (KV * GW))
    x = saved_ref[:, 0:GW].astype(f32)
    dx = inverse * (dq_ref[0] * gain_ref[...]) - x * (inverse * inverse * inverse * t)
    y_ref[...] = (grad_ref[...].astype(f32) + dx).astype(bf16)
    put_by_step(j, (out_0, out_1, out_2, out_3), y_ref)


def pool_sum_kernel(got_ref, out_ref, gain_ref):
    for g in range(KV):
        total = got_ref[g].astype(f32)
        for z in range(1, 8):
            total = total + got_ref[z * KV + g].astype(f32)
        cols = slice(g * HD, (g + 1) * HD)
        out_ref[0, :, cols] = total[0:64, :]
        out_ref[1, :, cols] = total[64:128, :]
        gain_ref[g] = total[128:136, :] + total[136:144, :]


def join_rows_kernel(member, *refs):
    out_ref = refs[KV]
    for r in range(KV):
        out_ref[:, group_at(member, r, GW)] = refs[r][...]


def join_own_kernel(member, *refs):
    out_ref = refs[KV]
    for r in range(KV):
        cols = group_at(member, r, HD)
        out_ref[0, :, cols] = refs[r][0:COMP, :]
        out_ref[1, :, cols] = refs[r][COMP : 2 * COMP, :]


smem = pl.BlockSpec(memory_space=pltpu.SMEM)
vmem = pl.BlockSpec(memory_space=pltpu.VMEM)


def whole(kernel, out_shape, in_specs):
    count = len(out_shape) if isinstance(out_shape, (list, tuple)) else None
    return pl.pallas_call(
        kernel,
        out_shape=out_shape,
        in_specs=in_specs,
        out_specs=[vmem] * count if count else vmem,
        interpret=INTERPRET,
    )


def shifted_to_group(values, steps):
    sections = lax.axis_size("section")
    got = []
    for r, value in enumerate(values):
        pairs = [
            (s * KV + k, ((s + steps) % sections) * KV + (k ^ r))
            for s in range(sections)
            for k in range(KV)
        ]
        got.append(lax.ppermute(value, ("section",) + QUAD, pairs))
    return got


def exchanged(values):
    pairs = lambda r: [(k, k ^ r) for k in range(KV)]
    return [values[0]] + [lax.ppermute(values[r], QUAD, pairs(r)) for r in range(1, KV)]


def to_all(tiles, axes):
    return lax.all_to_all(tiles, axes, 0, 0, tiled=True)


def by_member(shape):
    return pl.BlockSpec((1,) + shape, lambda j, *scalars: (j,) + (0,) * len(shape))


def fixed(shape):
    return pl.BlockSpec(shape, lambda j, *scalars: (0,) * len(shape))


t_spec = pl.BlockSpec((8, HD), lambda j, *scalars: (2 * COMP // 8, 0))
gain_spec = pl.BlockSpec((1, GW), lambda j, member, *scalars: (0, member[0]))


def over_members(kernel, scalars, in_specs, out_specs, out_shape, scratch, flops):
    return pl.pallas_call(
        kernel,
        out_shape=out_shape,
        grid_spec=pltpu.PrefetchScalarGridSpec(
            num_scalar_prefetch=scalars,
            grid=(KV,),
            in_specs=in_specs,
            out_specs=out_specs,
            scratch_shapes=scratch,
        ),
        compiler_params=pltpu.CompilerParams(dimension_semantics=("arbitrary",)),
        cost_estimate=pl.CostEstimate(flops=flops, transcendentals=0, bytes_accessed=4 << 20),
        interpret=INTERPRET,
    )


def shaped(shape, dtype):
    return jax.ShapeDtypeStruct(shape, dtype)


def section_tick(
    arriving,
    saved_input,
    returning,
    prompt_cache,
    fresh_cache,
    back_cache,
    query_gain,
    block_tables,
    fresh_lengths,
    back_lengths,
):
    places = [2 * lax.axis_index("fork_1") + lax.axis_index("fork_2"), lax.axis_index("fork_0")]
    member = jnp.stack(places).astype(jnp.int32)
    table = block_tables[0]
    keys = PROMPT + COMP
    four = range(KV)

    first = whole(
        pack_first_kernel, [shaped((FIRST_ROWS, HD), bf16)] * KV, [smem, vmem, vmem]
    )(member, prompt_cache[0], fresh_cache[0, 0])
    first = exchanged(first)
    incoming = whole(
        pack_arriving_kernel, [shaped((COMP, ARRIVE_W), bf16)] * KV, [smem, smem, vmem]
    )(member, fresh_lengths, arriving[0, 0])
    incoming = shifted_to_group(incoming, 1)
    slab = jnp.stack([part[0:HD] for part in first])
    slabs = {0: slab}
    for far in (1, 7, 2, 6, 3, 5, 4):
        slabs[far] = lax.ppermute(slab, "fork_0", [(z, (z + far) % 8) for z in range(8)])
    pool = jnp.stack([slabs[far] for far in range(8)]).reshape(32, HD, HD)

    saved = whole(
        pack_saved_kernel, [shaped((COMP, SAVED_W), bf16)] * KV, [smem, smem, vmem, vmem]
    )(member, back_lengths, saved_input[0, 0], back_cache[0, 0])
    saved = exchanged(saved)
    cotangent = whole(
        pack_returning_kernel, [shaped((COMP, GW), bf16)] * KV, [smem, vmem]
    )(member, returning[0, 0])
    cotangent = shifted_to_group(cotangent, -1)

    *output, prompt_k, prompt_v = over_members(
        forward_kernel,
        2,
        [fixed((32, HD, HD))]
        + [fixed((COMP, ARRIVE_W)) for _ in four]
        + [fixed((FIRST_ROWS, HD)) for _ in four]
        + [gain_spec],
        [fixed((COMP, GW)) for _ in four] + [fixed((PROMPT, HD)), fixed((PROMPT, HD))],
        [shaped((COMP, GW), bf16) for _ in four]
        + [shaped((PROMPT, HD), bf16), shaped((PROMPT, HD), bf16)],
        [
            pltpu.VMEM((COMP, ARRIVE_W), bf16),
            pltpu.VMEM((FIRST_ROWS, HD), bf16),
            pltpu.VMEM((keys, HD), bf16),
            pltpu.VMEM((HD, keys), bf16),
            pltpu.VMEM((HEADS // TOGETHER, keys, COLS), f32),
            pltpu.VMEM((HEADS // TOGETHER, keys, COLS), bf16),
            pltpu.VMEM((COMP, GW), bf16),
        ],
        4 * 4096 * keys * HD,
    )(member, table, pool, *incoming, *first, query_gain)
    output = exchanged(output)

    d_query, *own, reduced = over_members(
        backward_kernel,
        2,
        [fixed((COMP, SAVED_W)) for _ in four]
        + [fixed((COMP, GW)) for _ in four]
        + [fixed((PROMPT, HD)), fixed((PROMPT, HD)), gain_spec],
        [by_member((COMP, GW))]
        + [fixed((2 * COMP + 8, HD)) for _ in four]
        + [fixed((32, 144, HD))],
        [shaped((KV, COMP, GW), f32)]
        + [shaped((2 * COMP + 8, HD), f32) for _ in four]
        + [shaped((32, 144, HD), bf16)],
        [
            pltpu.VMEM((COMP, SAVED_W), bf16),
            pltpu.VMEM((COMP, GW), bf16),
            pltpu.VMEM((keys, HD), bf16),
            pltpu.VMEM((HD, keys), bf16),
            pltpu.VMEM((keys, HD), bf16),
            pltpu.VMEM((keys, HD), f32),
            pltpu.VMEM((keys, HD), f32),
            pltpu.VMEM((HEADS // TOGETHER, keys, COLS), f32),
            pltpu.VMEM((HEADS // TOGETHER, keys, COLS), f32),
            pltpu.VMEM((HEADS // TOGETHER, keys, COLS), bf16),
            pltpu.VMEM((HEADS, HD), f32),
            pltpu.VMEM((8, HD), f32),
        ],
        10 * 4096 * keys * HD,
    )(member, table, *saved, *cotangent, prompt_k, prompt_v, query_gain)

    own = exchanged(own)
    reduced = to_all(reduced, FORK)

    input_grad = over_members(
        input_grad_kernel,
        1,
        [by_member((COMP, GW))]
        + [fixed((COMP, SAVED_W)) for _ in four]
        + [fixed((COMP, GW)) for _ in four]
        + [gain_spec]
        + [t_spec for _ in four],
        [fixed((COMP, GW)) for _ in four],
        [shaped((COMP, GW), bf16) for _ in four],
        [
            pltpu.VMEM((COMP, GW), bf16),
            pltpu.VMEM((COMP, SAVED_W), bf16),
            pltpu.VMEM((COMP, GW), bf16),
        ],
        1 << 20,
    )(member, d_query, *saved, *cotangent, query_gain, *own)
    input_grad = exchanged(input_grad)

    prompt_grad, gain_grad = whole(
        pool_sum_kernel, [shaped((2, 64, KV * HD), f32), shaped((KV, HEADS, HD), f32)], [vmem]
    )(reduced)

    joined = [smem] + [vmem] * KV
    rows = shaped((COMP, KV * GW), bf16)
    own_grad = whole(join_own_kernel, shaped((2, COMP, KV * HD), f32), joined)(member, *own)
    output = whole(join_rows_kernel, rows, joined)(member, *output)
    input_grad = whole(join_rows_kernel, rows, joined)(member, *input_grad)
    return (
        output[None, None],
        input_grad[None, None],
        prompt_grad[None],
        own_grad[None, None],
        gain_grad.reshape(1, KV * GW),
    )


def solution(mesh):
    finer = Mesh(
        mesh.devices.reshape(mesh.shape["section"], 8, 2, 2),
        ("section", "fork_0", "fork_1", "fork_2"),
    )
    placed = (
        P("section", FORK, None, None),
        P("section", FORK, None, None),
        P("section", FORK, None, None),
        P("section", None, FORK, None),
        P("section", FORK, None, None, None),
        P("section", FORK, None, None, None),
        P("section", None),
        P(FORK, None),
        P(FORK),
        P(FORK),
    )
    return jax.shard_map(
        section_tick,
        mesh=finer,
        in_specs=placed,
        out_specs=(
            P("section", FORK, None, None),
            P("section", FORK, None, None),
            P("section", None, FORK, None),
            P("section", FORK, None, None, None),
            P("section", None),
        ),
        check_vma=False,
    )
```

```python
import jax
import jax.numpy as jnp
from jax import lax
from jax.experimental import pallas as pl
from jax.experimental.pallas import tpu as pltpu
from jax.sharding import Mesh
from jax.sharding import PartitionSpec as P

KV = 4
HD = 128
BLOCK = 16
COMP = 128
NB = 64
GW = 1024
HEADS = 8
PROMPT = NB * BLOCK
SCALE = HD ** (-0.5)
FORK = ("fork_0", "fork_1", "fork_2")
QUAD = ("fork_1", "fork_2")
INTERPRET = False


epsilon = 1e-06
masked_score = -1e30
bf16 = jnp.bfloat16
f32 = jnp.float32

NT = (((1,), (1,)), ((), ()))

OWN_K, OWN_V, STATS = 1024, 1152, 1280
SAVED_W = 1408
ARRIVE_W = 1152
FIRST_ROWS = 384


def nt_dot(a, b):
    return lax.dot_general(a, b, NT, preferred_element_type=f32)


def nn_dot(a, b):
    return jnp.dot(a, b, preferred_element_type=f32)


def stats_tile(x, length):
    floated = x.astype(f32)
    inverse = lax.rsqrt(jnp.mean(floated * floated, axis=-1, keepdims=True) + epsilon)
    high = inverse.astype(bf16).astype(f32)
    rest = inverse - high
    middle = rest.astype(bf16).astype(f32)
    low = rest - middle
    lane = lax.broadcasted_iota(jnp.int32, (x.shape[0], HD), 1)
    tile = jnp.where(lane == 0, high, jnp.where(lane == 1, middle, jnp.where(lane == 2, low, 0.0)))
    tile = jnp.where(lane == 3, length.astype(f32), tile)
    return tile.astype(bf16)


def read_stats(tile):
    t = tile.astype(f32)
    inverse = t[:, 0:1] + t[:, 1:2] + t[:, 2:3]
    return inverse, t[:, 3:4]


def group_at(member, r, width):
    return pl.ds(pl.multiple_of(jnp.bitwise_xor(member[0], r) * width, width), width)


def pack_first_kernel(member, pool_ref, fresh_ref, *out_refs):
    for r in range(KV):
        cols = group_at(member, r, HD)
        out_refs[r][0:64, :] = pool_ref[0, :, cols]
        out_refs[r][64:128, :] = pool_ref[1, :, cols]
        out_refs[r][128:256, :] = fresh_ref[0, :, cols]
        out_refs[r][256:384, :] = fresh_ref[1, :, cols]


def pack_saved_kernel(member, length, x_ref, back_ref, *out_refs):
    tile = stats_tile(x_ref[...], length[0])
    for r in range(KV):
        out_ref = out_refs[r]
        out_ref[:, 0:GW] = x_ref[:, group_at(member, r, GW)]
        cols = group_at(member, r, HD)
        out_ref[:, OWN_K : OWN_K + HD] = back_ref[0, :, cols]
        out_ref[:, OWN_V : OWN_V + HD] = back_ref[1, :, cols]
        out_ref[:, STATS : STATS + HD] = tile


def pack_returning_kernel(member, x_ref, *out_refs):
    for r in range(KV):
        out_refs[r][...] = x_ref[:, group_at(member, r, GW)]


def pack_arriving_kernel(member, length, x_ref, *out_refs):
    tile = stats_tile(x_ref[...], length[0])
    for r in range(KV):
        out_refs[r][:, 0:GW] = x_ref[:, group_at(member, r, GW)]
        out_refs[r][:, GW : GW + HD] = tile


TOGETHER = 4
COLS = TOGETHER * COMP
STEP = 64
NKEYS = PROMPT + COMP
NSTEP = NKEYS // STEP
LOG2E = 1.4426950408889634


def some_heads(rows, part):
    a = part * TOGETHER * HD
    return jnp.concatenate([rows[:, a + e * HD : a + (e + 1) * HD] for e in range(TOGETHER)], axis=0)


def own_mask(length):
    u = lax.broadcasted_iota(jnp.int32, (COMP, COLS), 0)
    i = lax.broadcasted_iota(jnp.int32, (COMP, COLS), 1) & (COMP - 1)
    return (u <= i) & (u.astype(f32) < length[0:1, 0:1])


def steps():
    return [slice(c * STEP, (c + 1) * STEP) for c in range(NSTEP)]


def softmax_columns(s_ref, mask):
    s_ref[PROMPT:, :] = jnp.where(mask, s_ref[PROMPT:, :], masked_score)
    top = None
    for rows in steps():
        part = jnp.max(s_ref[rows, :], axis=0, keepdims=True)
        top = part if top is None else jnp.maximum(top, part)
    top = top * (SCALE * LOG2E)
    total = None
    for rows in steps():
        p = jnp.exp2(s_ref[rows, :] * (SCALE * LOG2E) - top)
        s_ref[rows, :] = p
        part = jnp.sum(p, axis=0, keepdims=True)
        total = part if total is None else total + part
    return 1.0 / total


def put_by_step(j, out_refs, from_ref):
    for r in range(KV):

        @pl.when(j == r)
        def _(r=r):
            out_refs[r][...] = from_ref[...]


def take_by_step(j, from_refs, to_ref):
    for r in range(KV):

        @pl.when(j == r)
        def _(r=r):
            to_ref[...] = from_refs[r][...]


def backward_kernel(
    member, table, saved_0, saved_1, saved_2, saved_3, grad_0, grad_1, grad_2, grad_3,
    prompt_k_ref, prompt_v_ref, gain_ref,
    dq_ref, own_0, own_1, own_2, own_3, reduce_ref,
    saved_ref, grad_ref,
    keys_ref, keys_t_ref, values_ref, dk_ref, dv_ref, s_refs, w_refs, b_refs, gain_acc, t_ref,
):
    j = pl.program_id(0)
    own_refs = (own_0, own_1, own_2, own_3)
    take_by_step(j, (saved_0, saved_1, saved_2, saved_3), saved_ref)
    take_by_step(j, (grad_0, grad_1, grad_2, grad_3), grad_ref)

    @pl.when(j == 0)
    def _():
        keys_ref[0:PROMPT, :] = prompt_k_ref[...]
        values_ref[0:PROMPT, :] = prompt_v_ref[...]
        for c in range(PROMPT // HD):
            rows = slice(c * HD, (c + 1) * HD)
            keys_t_ref[:, rows] = keys_ref[rows, :].astype(f32).T.astype(bf16)
        dk_ref[0:PROMPT, :] = jnp.zeros((PROMPT, HD), f32)
        dv_ref[0:PROMPT, :] = jnp.zeros((PROMPT, HD), f32)
        gain_acc[...] = jnp.zeros(gain_acc.shape, f32)

    inverse, length = read_stats(saved_ref[:, STATS : STATS + HD])
    x = saved_ref[:, 0:GW].astype(f32)
    normal = x * inverse
    gain = gain_ref[...]
    q = (normal * gain).astype(bf16)
    row = lax.broadcasted_iota(jnp.int32, (COMP, 1), 0).astype(f32)
    valid = row < length
    d_out = jnp.where(valid, grad_ref[...].astype(f32), 0.0).astype(bf16)
    keys_ref[PROMPT:, :] = saved_ref[:, OWN_K : OWN_K + HD]
    values_ref[PROMPT:, :] = saved_ref[:, OWN_V : OWN_V + HD]
    keys_t_ref[:, PROMPT:] = saved_ref[:, OWN_K : OWN_K + HD].astype(f32).T.astype(bf16)
    dk_ref[PROMPT:, :] = jnp.zeros((COMP, HD), f32)
    dv_ref[PROMPT:, :] = jnp.zeros((COMP, HD), f32)
    mask = own_mask(length)

    t = jnp.zeros((COMP, 1), f32)
    for part in range(HEADS // TOGETHER):
        s_refs[part, :, :] = nt_dot(keys_ref[...], some_heads(q, part))
        w_refs[part, :, :] = nt_dot(values_ref[...], some_heads(d_out, part))
    for part in range(HEADS // TOGETHER):
        q_rows = some_heads(q, part)
        d_rows = some_heads(d_out, part)
        s_ref, w_ref, b_ref = s_refs.at[part], w_refs.at[part], b_refs.at[part]
        ratio = softmax_columns(s_ref, mask)
        delta = None
        for rows in steps():
            a = s_ref[rows, :] * ratio
            s_ref[rows, :] = a
            b_ref[rows, :] = a.astype(bf16)
            piece = jnp.sum(a * w_ref[rows, :], axis=0, keepdims=True)
            delta = piece if delta is None else delta + piece
        dv_ref[...] += nn_dot(b_ref[...], d_rows)
        for rows in steps():
            b_ref[rows, :] = (s_ref[rows, :] * (w_ref[rows, :] - delta) * SCALE).astype(bf16)
        dk_ref[...] += nn_dot(b_ref[...], q_rows)
        dq_t = nn_dot(keys_t_ref[...], b_ref[...])
        for e in range(TOGETHER):
            h = TOGETHER * part + e
            cols = slice(h * HD, (h + 1) * HD)
            dq = dq_t[:, e * HD : (e + 1) * HD].T
            dq_ref[0, :, cols] = dq
            t = t + jnp.sum(dq * gain[:, cols] * x[:, cols], axis=1, keepdims=True)
            gain_acc[h : h + 1, :] += jnp.sum(dq * normal[:, cols], axis=0, keepdims=True)

    for r in range(KV):

        @pl.when(j == r)
        def _(r=r):
            own_refs[r][0:COMP, :] = dk_ref[PROMPT:, :]
            own_refs[r][COMP : 2 * COMP, :] = dv_ref[PROMPT:, :]

    @pl.when(j == 0)
    def _():
        t_ref[...] = jnp.zeros((8, HD), f32)

    place = lax.broadcasted_iota(jnp.int32, (8, HD), 0)
    t_rows = jnp.broadcast_to(t, (COMP, HD)).T[0:8, :]
    t_ref[...] = jnp.where(place == jnp.bitwise_xor(j, member[0]), t_rows, t_ref[...])

    @pl.when(j == KV - 1)
    def _():
        for own_ref in own_refs:
            own_ref[2 * COMP :, :] = t_ref[...]
        high = gain_acc[...].astype(bf16)
        low = (gain_acc[...] - high.astype(f32)).astype(bf16)
        both = jnp.concatenate([high, low], axis=0)

        def clear(n, carry):
            reduce_ref[n, 0:HD, :] = jnp.zeros((HD, HD), bf16)
            reduce_ref[n, HD : HD + 16, :] = both
            return carry

        lax.fori_loop(0, 32, clear, 0)

        def spread(n, carry):
            b = table[n]
            holder = b // 4
            at = pl.multiple_of((b % 4) * BLOCK, BLOCK)
            start = pl.multiple_of(n * BLOCK, BLOCK)
            reduce_ref[holder, pl.ds(at, BLOCK), :] = dk_ref[pl.ds(start, BLOCK), :].astype(bf16)
            reduce_ref[holder, pl.ds(at + 64, BLOCK), :] = dv_ref[pl.ds(start, BLOCK), :].astype(bf16)
            return carry

        lax.fori_loop(0, NB, spread, 0)


def forward_kernel(
    member, table, pool_ref, arrive_0, arrive_1, arrive_2, arrive_3,
    first_0, first_1, first_2, first_3, gain_ref,
    out_0, out_1, out_2, out_3, prompt_k_ref, prompt_v_ref,
    arrive_ref, first_ref, keys_ref, values_t_ref, s_refs, b_refs, y_ref,
):
    j = pl.program_id(0)
    take_by_step(j, (arrive_0, arrive_1, arrive_2, arrive_3), arrive_ref)
    take_by_step(j, (first_0, first_1, first_2, first_3), first_ref)

    @pl.when(j == 0)
    def _():
        def pick(n, carry):
            b = table[n]
            place = (b // 16) * KV + jnp.bitwise_xor((b // 4) % 4, member[0])
            at = pl.multiple_of((b % 4) * BLOCK, BLOCK)
            to = pl.multiple_of(n * BLOCK, BLOCK)
            prompt_k_ref[pl.ds(to, BLOCK), :] = pool_ref[place, pl.ds(at, BLOCK), :]
            prompt_v_ref[pl.ds(to, BLOCK), :] = pool_ref[place, pl.ds(at + 64, BLOCK), :]
            return carry

        lax.fori_loop(0, NB, pick, 0)
        keys_ref[0:PROMPT, :] = prompt_k_ref[...]
        for c in range(PROMPT // HD):
            rows = slice(c * HD, (c + 1) * HD)
            values_t_ref[:, rows] = prompt_v_ref[rows, :].astype(f32).T.astype(bf16)

    inverse, length = read_stats(arrive_ref[:, GW : GW + HD])
    x = arrive_ref[:, 0:GW].astype(f32)
    q = (x * inverse * gain_ref[...]).astype(bf16)
    row = lax.broadcasted_iota(jnp.int32, (COMP, 1), 0).astype(f32)
    valid = row < length
    keys_ref[PROMPT:, :] = first_ref[128:256, :]
    values_t_ref[:, PROMPT:] = first_ref[256:384, :].astype(f32).T.astype(bf16)
    mask = own_mask(length)
    for part in range(HEADS // TOGETHER):
        s_refs[part, :, :] = nt_dot(keys_ref[...], some_heads(q, part))
    for part in range(HEADS // TOGETHER):
        s_ref, b_ref = s_refs.at[part], b_refs.at[part]
        ratio = softmax_columns(s_ref, mask)
        for rows in steps():
            b_ref[rows, :] = (s_ref[rows, :] * ratio).astype(bf16)
        o_t = nn_dot(values_t_ref[...], b_ref[...])
        for e in range(TOGETHER):
            h = TOGETHER * part + e
            cols = slice(h * HD, (h + 1) * HD)
            o = jnp.where(valid, o_t[:, e * HD : (e + 1) * HD].T, 0.0)
            y_ref[:, cols] = (x[:, cols] + o).astype(bf16)
    put_by_step(j, (out_0, out_1, out_2, out_3), y_ref)


def input_grad_kernel(
    member, dq_ref, saved_0, saved_1, saved_2, saved_3, grad_0, grad_1, grad_2, grad_3,
    gain_ref, t_0, t_1, t_2, t_3, out_0, out_1, out_2, out_3, y_ref, saved_ref, grad_ref
):
    j = pl.program_id(0)
    take_by_step(j, (saved_0, saved_1, saved_2, saved_3), saved_ref)
    take_by_step(j, (grad_0, grad_1, grad_2, grad_3), grad_ref)
    inverse, _ = read_stats(saved_ref[:, STATS : STATS + HD])
    total = t_0[...] + t_1[...] + t_2[...] + t_3[...]
    place = lax.broadcasted_iota(jnp.int32, (8, HD), 0)
    t_row = jnp.sum(jnp.where(place == jnp.bitwise_xor(j, member[0]), total, 0.0), axis=0, keepdims=True)
    t = jnp.broadcast_to(t_row, (HD, HD)).T[:, 0:1] * (1.0 / (KV * GW))
    x = saved_ref[:, 0:GW].astype(f32)
    dx = inverse * (dq_ref[0] * gain_ref[...]) - x * (inverse * inverse * inverse * t)
    y_ref[...] = (grad_ref[...].astype(f32) + dx).astype(bf16)
    put_by_step(j, (out_0, out_1, out_2, out_3), y_ref)


def pool_sum_kernel(got_ref, out_ref, gain_ref):
    for g in range(KV):
        total = got_ref[g].astype(f32)
        for z in range(1, 8):
            total = total + got_ref[z * KV + g].astype(f32)
        cols = slice(g * HD, (g + 1) * HD)
        out_ref[0, :, cols] = total[0:64, :]
        out_ref[1, :, cols] = total[64:128, :]
        gain_ref[g] = total[128:136, :] + total[136:144, :]


def join_rows_kernel(member, *refs):
    out_ref = refs[KV]
    for r in range(KV):
        out_ref[:, group_at(member, r, GW)] = refs[r][...]


def join_own_kernel(member, *refs):
    out_ref = refs[KV]
    for r in range(KV):
        cols = group_at(member, r, HD)
        out_ref[0, :, cols] = refs[r][0:COMP, :]
        out_ref[1, :, cols] = refs[r][COMP : 2 * COMP, :]


smem = pl.BlockSpec(memory_space=pltpu.SMEM)
vmem = pl.BlockSpec(memory_space=pltpu.VMEM)


def whole(kernel, out_shape, in_specs):
    count = len(out_shape) if isinstance(out_shape, (list, tuple)) else None
    return pl.pallas_call(
        kernel,
        out_shape=out_shape,
        in_specs=in_specs,
        out_specs=[vmem] * count if count else vmem,
        interpret=INTERPRET,
    )


def shifted_to_group(values, steps):
    sections = lax.axis_size("section")
    got = []
    for r, value in enumerate(values):
        pairs = [
            (s * KV + k, ((s + steps) % sections) * KV + (k ^ r))
            for s in range(sections)
            for k in range(KV)
        ]
        got.append(lax.ppermute(value, ("section",) + QUAD, pairs))
    return got


def exchanged(values):
    pairs = lambda r: [(k, k ^ r) for k in range(KV)]
    return [values[0]] + [lax.ppermute(values[r], QUAD, pairs(r)) for r in range(1, KV)]


def to_all(tiles, axes):
    return lax.all_to_all(tiles, axes, 0, 0, tiled=True)


def by_member(shape):
    return pl.BlockSpec((1,) + shape, lambda j, *scalars: (j,) + (0,) * len(shape))


def fixed(shape):
    return pl.BlockSpec(shape, lambda j, *scalars: (0,) * len(shape))


t_spec = pl.BlockSpec((8, HD), lambda j, *scalars: (2 * COMP // 8, 0))
gain_spec = pl.BlockSpec((1, GW), lambda j, member, *scalars: (0, member[0]))


def over_members(kernel, scalars, in_specs, out_specs, out_shape, scratch, flops):
    return pl.pallas_call(
        kernel,
        out_shape=out_shape,
        grid_spec=pltpu.PrefetchScalarGridSpec(
            num_scalar_prefetch=scalars,
            grid=(KV,),
            in_specs=in_specs,
            out_specs=out_specs,
            scratch_shapes=scratch,
        ),
        compiler_params=pltpu.CompilerParams(dimension_semantics=("arbitrary",)),
        cost_estimate=pl.CostEstimate(flops=flops, transcendentals=0, bytes_accessed=4 << 20),
        interpret=INTERPRET,
    )


def shaped(shape, dtype):
    return jax.ShapeDtypeStruct(shape, dtype)


def section_tick(
    arriving,
    saved_input,
    returning,
    prompt_cache,
    fresh_cache,
    back_cache,
    query_gain,
    block_tables,
    fresh_lengths,
    back_lengths,
):
    member = (2 * lax.axis_index("fork_1") + lax.axis_index("fork_2")).astype(jnp.int32)[None]
    table = block_tables[0]
    keys = PROMPT + COMP
    four = range(KV)

    first = whole(
        pack_first_kernel, [shaped((FIRST_ROWS, HD), bf16)] * KV, [smem, vmem, vmem]
    )(member, prompt_cache[0], fresh_cache[0, 0])
    first = exchanged(first)
    incoming = whole(
        pack_arriving_kernel, [shaped((COMP, ARRIVE_W), bf16)] * KV, [smem, smem, vmem]
    )(member, fresh_lengths, arriving[0, 0])
    incoming = shifted_to_group(incoming, 1)
    slab = jnp.stack([part[0:HD] for part in first])
    slabs = jnp.broadcast_to(slab[None], (8, KV, HD, HD))
    pool = to_all(slabs, "fork_0").reshape(32, HD, HD)

    saved = whole(
        pack_saved_kernel, [shaped((COMP, SAVED_W), bf16)] * KV, [smem, smem, vmem, vmem]
    )(member, back_lengths, saved_input[0, 0], back_cache[0, 0])
    saved = exchanged(saved)
    cotangent = whole(
        pack_returning_kernel, [shaped((COMP, GW), bf16)] * KV, [smem, vmem]
    )(member, returning[0, 0])
    cotangent = shifted_to_group(cotangent, -1)

    *output, prompt_k, prompt_v = over_members(
        forward_kernel,
        2,
        [fixed((32, HD, HD))]
        + [fixed((COMP, ARRIVE_W)) for _ in four]
        + [fixed((FIRST_ROWS, HD)) for _ in four]
        + [gain_spec],
        [fixed((COMP, GW)) for _ in four] + [fixed((PROMPT, HD)), fixed((PROMPT, HD))],
        [shaped((COMP, GW), bf16) for _ in four]
        + [shaped((PROMPT, HD), bf16), shaped((PROMPT, HD), bf16)],
        [
            pltpu.VMEM((COMP, ARRIVE_W), bf16),
            pltpu.VMEM((FIRST_ROWS, HD), bf16),
            pltpu.VMEM((keys, HD), bf16),
            pltpu.VMEM((HD, keys), bf16),
            pltpu.VMEM((HEADS // TOGETHER, keys, COLS), f32),
            pltpu.VMEM((HEADS // TOGETHER, keys, COLS), bf16),
            pltpu.VMEM((COMP, GW), bf16),
        ],
        4 * 4096 * keys * HD,
    )(member, table, pool, *incoming, *first, query_gain)
    output = exchanged(output)

    d_query, *own, reduced = over_members(
        backward_kernel,
        2,
        [fixed((COMP, SAVED_W)) for _ in four]
        + [fixed((COMP, GW)) for _ in four]
        + [fixed((PROMPT, HD)), fixed((PROMPT, HD)), gain_spec],
        [by_member((COMP, GW))]
        + [fixed((2 * COMP + 8, HD)) for _ in four]
        + [fixed((32, 144, HD))],
        [shaped((KV, COMP, GW), f32)]
        + [shaped((2 * COMP + 8, HD), f32) for _ in four]
        + [shaped((32, 144, HD), bf16)],
        [
            pltpu.VMEM((COMP, SAVED_W), bf16),
            pltpu.VMEM((COMP, GW), bf16),
            pltpu.VMEM((keys, HD), bf16),
            pltpu.VMEM((HD, keys), bf16),
            pltpu.VMEM((keys, HD), bf16),
            pltpu.VMEM((keys, HD), f32),
            pltpu.VMEM((keys, HD), f32),
            pltpu.VMEM((HEADS // TOGETHER, keys, COLS), f32),
            pltpu.VMEM((HEADS // TOGETHER, keys, COLS), f32),
            pltpu.VMEM((HEADS // TOGETHER, keys, COLS), bf16),
            pltpu.VMEM((HEADS, HD), f32),
            pltpu.VMEM((8, HD), f32),
        ],
        10 * 4096 * keys * HD,
    )(member, table, *saved, *cotangent, prompt_k, prompt_v, query_gain)

    own = exchanged(own)
    reduced = to_all(reduced, FORK)

    input_grad = over_members(
        input_grad_kernel,
        1,
        [by_member((COMP, GW))]
        + [fixed((COMP, SAVED_W)) for _ in four]
        + [fixed((COMP, GW)) for _ in four]
        + [gain_spec]
        + [t_spec for _ in four],
        [fixed((COMP, GW)) for _ in four],
        [shaped((COMP, GW), bf16) for _ in four],
        [
            pltpu.VMEM((COMP, GW), bf16),
            pltpu.VMEM((COMP, SAVED_W), bf16),
            pltpu.VMEM((COMP, GW), bf16),
        ],
        1 << 20,
    )(member, d_query, *saved, *cotangent, query_gain, *own)
    input_grad = exchanged(input_grad)

    prompt_grad, gain_grad = whole(
        pool_sum_kernel, [shaped((2, 64, KV * HD), f32), shaped((KV, HEADS, HD), f32)], [vmem]
    )(reduced)

    joined = [smem] + [vmem] * KV
    rows = shaped((COMP, KV * GW), bf16)
    own_grad = whole(join_own_kernel, shaped((2, COMP, KV * HD), f32), joined)(member, *own)
    output = whole(join_rows_kernel, rows, joined)(member, *output)
    input_grad = whole(join_rows_kernel, rows, joined)(member, *input_grad)
    return (
        output[None, None],
        input_grad[None, None],
        prompt_grad[None],
        own_grad[None, None],
        gain_grad.reshape(1, KV * GW),
    )


def solution(mesh):
    finer = Mesh(
        mesh.devices.reshape(mesh.shape["section"], 8, 2, 2),
        ("section", "fork_0", "fork_1", "fork_2"),
    )
    placed = (
        P("section", FORK, None, None),
        P("section", FORK, None, None),
        P("section", FORK, None, None),
        P("section", None, FORK, None),
        P("section", FORK, None, None, None),
        P("section", FORK, None, None, None),
        P("section", None),
        P(FORK, None),
        P(FORK),
        P(FORK),
    )
    return jax.shard_map(
        section_tick,
        mesh=finer,
        in_specs=placed,
        out_specs=(
            P("section", FORK, None, None),
            P("section", FORK, None, None),
            P("section", None, FORK, None),
            P("section", FORK, None, None, None),
            P("section", None),
        ),
        check_vma=False,
    )
```
